32 devices in a mesh: row: 8 (over z, y), col: 4 (over x, core).
Axes of the slice: x: 2, y: 2, z: 4, core: 2. Of those that a mesh axis runs over, the one named last changes fastest.
Arguments:
- load_currents: float32 [32, 1024, 512], P(None, 'row', 'col'), may hold values from -36 to 36
- labels: int32 [1024, 512], P('row', 'col'), may hold values from 0 to 255, as said below
- bump_height: float32 [1024, 512], P('row', 'col'), may hold values from 0.5 to 2
- horizontal_class: int32 [1024, 512], P('row', 'col'), may hold values from 0 to 7
- vertical_class: int32 [1024, 512], P('row', 'col'), may hold values from 0 to 7
- pad_class: int32 [1024, 512], P('row', 'col'), may hold values from 0 to 7
- edge_table: float32 [8], replicated, may hold values from 0.5 to 4
- pad_table: float32 [8], replicated, may hold values from 0.02 to 0.5
Outputs:
- solution: float32 [32, 1024, 512], P(None, 'row', 'col')
- residual: float32 [32, 1024, 512], P(None, 'row', 'col')
The draws below stay inside these ranges and needn't reach their ends.
Inputs may be any that keep to these rules, and one draw needn't show every extreme that they name: `labels`: every number from 0 to 255 is the label of some nodes; the label of node (i, j) is 16 * floor(16 * i2 / 1024) + floor(16 * j2 / 512) for some node (i2, j2) of the grid with |i2 - i| <= 16 and |j2 - j| <= 8.
All inputs are finite; a program needn't handle non-finite values.
Results may differ from the reference program's by a relative error of at most 0.0003.
Values sent between devices are 32-bit elements; how exact they have to be, the bound alone decides.
A program may use at most 128 MiB of HBM per device.

```python
import math
from functools import partial
import jax
import jax.numpy as jnp
from jax import lax

NRHS = 32
REG = 16
NCLS = 8
ITERS = 2
NX = 1024
NY = 512


def draw_labels(key, part):
    first_key, second_key = jax.random.split(jax.random.fold_in(key, 17))
    reach_rows = NX // (4 * REG)
    reach_cols = NY // (4 * REG)
    row_shift = jax.random.randint(first_key, (NX, NY), -reach_rows, reach_rows + 1)
    col_shift = jax.random.randint(second_key, (NX, NY), -reach_cols, reach_cols + 1)
    rows_index = jnp.arange(NX, dtype=jnp.int32)[:, None] + row_shift
    columns = jnp.arange(NY, dtype=jnp.int32)[None, :] + col_shift
    row_block = jnp.clip(rows_index * REG // NX, 0, REG - 1)
    col_block = jnp.clip(columns * REG // NY, 0, REG - 1)
    return (row_block * REG + col_block).astype(jnp.int32)


def draw_load_currents(key, part):
    rows_index = jnp.arange(NX, dtype=jnp.float32)[:, None]
    rising = 1.0 + 2.0 * rows_index / max(NX - 1, 1)
    normal_part = jnp.clip(jax.random.normal(jax.random.fold_in(key, 5), (NRHS, NX, NY), jnp.float32), -6.0, 6.0)
    return 2.0 * normal_part * rising


def set_ends(entries, own_key, low, largest):
    longest = entries.shape.index(max(entries.shape))
    spots = []
    for shift in (0, 1):
        where = [jax.random.randint(jax.random.fold_in(own_key, axis), (), 0, length) for axis, length in enumerate(entries.shape)]
        where[longest] = (where[longest] + shift) % entries.shape[longest]
        spots.append(tuple(where))
    return entries.at[spots[0]].set(low).at[spots[1]].set(largest)


def steps_of(own_key, dims, pieces, smallest, top_value):
    level, own = 1.0, jax.random.fold_in(own_key, 6)
    for axis_at, parts in pieces:
        steps = jnp.exp(jax.random.uniform(jax.random.fold_in(own, axis_at), (parts,), jnp.float32, smallest / len(pieces), top_value / len(pieces)))
        level = level * jnp.repeat(steps, dims[axis_at] // parts).reshape([-1 if axis == axis_at else 1 for axis in range(len(dims))])
    return level


def setup_inputs(seed: int = 0) -> dict:
    splits = jax.random.split(jax.random.key(seed), 9)
    load_currents = draw_load_currents(jax.random.fold_in(splits[8], 71), 0)
    labels = draw_labels(jax.random.fold_in(splits[8], 71), 0)
    bump_height = jnp.clip(jnp.exp(math.log(2.0) - 1.3862944 * jax.random.uniform(splits[2], (NX, NY), jnp.float32) ** steps_of(splits[2], (NX, NY), ((0, 8), (1, 4)), -0.2, 0.2)), 0.5, 2.0)
    horizontal_class = set_ends(jax.random.randint(splits[3], (NX, NY), 0, NCLS), jax.random.fold_in(splits[3], 1), 0, NCLS - 1).astype(jnp.int32)
    vertical_class = set_ends(jax.random.randint(splits[4], (NX, NY), 0, NCLS), jax.random.fold_in(splits[4], 1), 0, NCLS - 1).astype(jnp.int32)
    pad_class = set_ends(jax.random.randint(splits[5], (NX, NY), 0, NCLS), jax.random.fold_in(splits[5], 1), 0, NCLS - 1).astype(jnp.int32)
    edge_table = jnp.clip(jnp.exp(jax.random.uniform(splits[6], (NCLS,), jnp.float32, math.log(0.5), math.log(4.0))), 0.5, 4.0)
    pad_table = jnp.clip(jnp.exp(jax.random.uniform(splits[7], (NCLS,), jnp.float32, math.log(0.02), math.log(0.5))), 0.02, 0.5)
    return {"load_currents": load_currents, "labels": labels, "bump_height": bump_height, "horizontal_class": horizontal_class, "vertical_class": vertical_class, "pad_class": pad_class, "edge_table": edge_table, "pad_table": pad_table}


precise = lax.Precision.HIGHEST

def link_fields(horizontal_class, vertical_class, edge_table):
    right_link = edge_table[horizontal_class]
    down_link = edge_table[vertical_class]
    columns = lax.broadcasted_iota(jnp.int32, horizontal_class.shape, 1)
    rows_index = lax.broadcasted_iota(jnp.int32, horizontal_class.shape, 0)
    right_link = jnp.where(columns == horizontal_class.shape[1] - 1, 0.0, right_link)
    down_link = jnp.where(rows_index == horizontal_class.shape[0] - 1, 0.0, down_link)
    left_link = jnp.pad(right_link, ((0, 0), (1, 0)))[:, :-1]
    upper_link = jnp.pad(down_link, ((1, 0), (0, 0)))[:-1, :]
    return (right_link, left_link, down_link, upper_link)

def apply_operator(field, coeffs):
    diagonal, right_link, left_link, down_link, upper_link = coeffs
    padded = jnp.pad(field, 1)
    return diagonal * field - right_link * padded[1:-1, 2:] - left_link * padded[1:-1, :-2] - down_link * padded[2:, 1:-1] - upper_link * padded[:-2, 1:-1]

def assemble_coarse(labels, bump_height, coeffs, regions):
    diagonal, right_link, left_link, down_link, upper_link = coeffs
    right_label = jnp.roll(labels, -1, axis=1)
    right_bump = jnp.roll(bump_height, -1, axis=1)
    down_label = jnp.roll(labels, -1, axis=0)
    down_bump = jnp.roll(bump_height, -1, axis=0)
    pair_ids = jnp.concatenate([(labels * regions + labels).reshape(-1), (labels * regions + right_label).reshape(-1), (right_label * regions + labels).reshape(-1), (labels * regions + down_label).reshape(-1), (down_label * regions + labels).reshape(-1)]).astype(jnp.int32)
    across = -(right_link * bump_height * right_bump)
    downward = -(down_link * bump_height * down_bump)
    weights = jnp.concatenate([(diagonal * bump_height * bump_height).reshape(-1), across.reshape(-1), across.reshape(-1), downward.reshape(-1), downward.reshape(-1)])
    summed = jax.ops.segment_sum(weights, pair_ids, num_segments=regions * regions)
    return summed.reshape(regions, regions)

def invert(matrix):
    factor = jnp.linalg.cholesky(matrix)
    identity = jnp.eye(matrix.shape[0], dtype=matrix.dtype)
    lower_solved = lax.linalg.triangular_solve(factor, identity, left_side=True, lower=True)
    return lax.linalg.triangular_solve(factor, lower_solved, left_side=True, lower=True, transpose_a=True)

def solve_single(single_load, labels, bump_height, coeffs, inverse, regions):
    flat_labels = labels.reshape(-1).astype(jnp.int32)
    diagonal = coeffs[0]

    def project(field):
        return jax.ops.segment_sum((bump_height * field).reshape(-1), flat_labels, num_segments=regions)

    def expand(coarse):
        return bump_height * jnp.take(coarse, labels, axis=0)

    def solve_coarse(projected):
        return jnp.dot(projected, inverse, precision=precise)

    def refresh(residual):
        scaled = residual / diagonal
        weighted_norm = jnp.sum(residual * scaled)
        field_image = apply_operator(scaled, coeffs)
        coarse = solve_coarse(project(field_image))
        return (scaled, weighted_norm, field_image, coarse)
    solution = expand(solve_coarse(project(single_load)))
    residual = single_load - apply_operator(solution, coeffs)
    scaled, weighted_norm, field_image, coarse = refresh(residual)
    spread = expand(coarse)
    direction = scaled - spread
    direction_image = field_image - apply_operator(spread, coeffs)
    for iteration in range(ITERS):
        step_size = weighted_norm / jnp.sum(direction * direction_image)
        solution = solution + step_size * direction
        residual = residual - step_size * direction_image
        if iteration + 1 < ITERS:
            scaled, new_norm, field_image, coarse = refresh(residual)
            spread = expand(coarse)
            beta_ratio = new_norm / weighted_norm
            direction = scaled - spread + beta_ratio * direction
            direction_image = field_image - apply_operator(spread, coeffs) + beta_ratio * direction_image
            weighted_norm = new_norm
    return (solution, residual)

def reference(load_currents, labels, bump_height, horizontal_class, vertical_class, pad_class, edge_table, pad_table):
    right_link, left_link, down_link, upper_link = link_fields(horizontal_class, vertical_class, edge_table)
    diagonal = pad_table[pad_class] + right_link + left_link + down_link + upper_link
    coeffs = (diagonal, right_link, left_link, down_link, upper_link)
    regions = REG * REG
    inverse = invert(assemble_coarse(labels, bump_height, coeffs, regions))
    worker = partial(solve_single, labels=labels, bump_height=bump_height, coeffs=coeffs, inverse=inverse, regions=regions)
    solution, residual = lax.map(worker, load_currents)
    return (solution, residual)
```

```python
import functools

import jax
import jax.numpy as jnp
from jax import lax
from jax.experimental import pallas as pl
from jax.experimental.pallas import tpu as pltpu
from jax.sharding import PartitionSpec as P

REG = 16
F32 = jnp.float32
precise = lax.Precision.HIGHEST
VM = pl.BlockSpec(memory_space=pltpu.VMEM)
SM = pl.BlockSpec(memory_space=pltpu.SMEM)
ANY = pl.BlockSpec(memory_space=pl.ANY)
BLOCK = 32
LANES = 4 * BLOCK
PITCH = 8
MINV, Z, W0, W1, W2, V0, V1, CO = 0, 1, 5, 9, 13, 17, 21, 25
KEPT, PLANES = 17, 30
ORDER = (0, 2, 4, 6, 8, 10, 12, 14, 1, 5, 9, 13, 3, 11, 7, 15)


def shape(*dims):
    return jax.ShapeDtypeStruct(dims, F32)


def iota(dims, axis):
    return lax.broadcasted_iota(jnp.int32, dims, axis)


def rolled(value, shift, axis):
    shift = shift % value.shape[axis]
    return pltpu.roll(value, shift, axis) if shift else value


class Plan:
    def __init__(self, rows, cols, loads, height, width, row_devices, col_devices):
        self.rows, self.cols, self.loads = rows, cols, loads
        self.height, self.width = height, width
        self.nr, self.nc = row_devices, col_devices
        self.count = row_devices * col_devices
        self.lv, self.cw = rows // height, cols // width
        self.parts = self.lv + 1
        self.levels = self.lv + 2
        self.half = loads // 2
        self.pitch = rows + PITCH

    def chunks(self):
        half = self.height // 2
        for part in range(self.parts):
            yield part, max(0, part * self.height - half), min(self.rows, part * self.height + half)


def over_rows(first, last, step, init, group=4):
    def body(g, carry):
        for u in range(group):
            carry = step(first + g * group + u, u, carry)
        return carry

    return lax.fori_loop(0, (last - first) // group, body, init)


def row_of(ref, k, i):
    return ref[k, pl.ds(i, 1), :]


class Legs:
    def __init__(self, plan, send_sem, recv_sem):
        self.plan, self.send_sem, self.recv_sem = plan, send_sem, recv_sem
        self.used = 0
        self.r, self.c = lax.axis_index("row"), lax.axis_index("col")
        self.everything = []

    def inside(self, dr, dc):
        r, c = self.r + dr, self.c + dc
        return (r >= 0) & (r < self.plan.nr) & (c >= 0) & (c < self.plan.nc)

    def make(self, items):
        out = []
        for dr, dc, src, dst in items:
            target = (lax.rem(self.r + dr + self.plan.nr, self.plan.nr), lax.rem(self.c + dc + self.plan.nc, self.plan.nc))
            copy = pltpu.make_async_remote_copy(
                src_ref=src,
                dst_ref=dst,
                send_sem=self.send_sem.at[self.used],
                recv_sem=self.recv_sem.at[self.used],
                device_id=target,
                device_id_type=pl.DeviceIdType.MESH,
            )
            self.used += 1
            out.append((self.inside(dr, dc), self.inside(-dr, -dc), copy))
        self.everything += out
        return out

    def start(self, legs):
        for goes, _, copy in legs:
            pl.when(goes)(copy.start)

    def wait(self, legs):
        for _, comes, copy in legs:
            pl.when(comes)(copy.wait_recv)

    def finish(self):
        for goes, _, copy in self.everything:
            pl.when(goes)(copy.wait_send)


def beside(src, dst):
    return [(1, 0, src.at[0], dst.at[0]), (-1, 0, src.at[1], dst.at[1]), (0, 1, src.at[2], dst.at[2]), (0, -1, src.at[3], dst.at[3])]


def looked_up(table_ref, classes):
    out = jnp.zeros(classes.shape, F32)
    for k in range(table_ref.shape[0]):
        out = jnp.where(classes == k, table_ref[k], out)
    return out


def put_edges(ref, k, value, row_end=True):
    rows, cols = value.shape
    ref[0, k : k + 1, :] = value[rows - 1 :]
    ref[1, k : k + 1, :] = value[:1]
    turned = value.T
    ref[2, k : k + 1, :] = turned[cols - 1 :]
    ref[3, k : k + 1, :] = turned[:1]


class Around:
    def __init__(self, edge_ref, rows, cols):
        self.edge_ref, self.rows, self.cols = edge_ref, rows, cols
        self.i, self.j = iota((rows, cols), 0), iota((rows, cols), 1)

    def column(self, side, k):
        return jnp.broadcast_to(self.edge_ref[side, k : k + 1, :], (self.cols, self.rows)).T

    def left(self, value, k):
        return jnp.where(self.j == 0, self.column(2, k), pltpu.roll(value, 1, 1))

    def right(self, value, k):
        return jnp.where(self.j == self.cols - 1, self.column(3, k), pltpu.roll(value, self.cols - 1, 1))

    def top(self, value, k):
        return jnp.where(self.i == 0, self.edge_ref[0, k : k + 1, :], pltpu.roll(value, 1, 0))

    def low(self, value, k):
        return jnp.where(self.i == self.rows - 1, self.edge_ref[1, k : k + 1, :], pltpu.roll(value, self.rows - 1, 0))

    def turns(self, at, size, step):
        out = None
        for p in range(1, size // step + 1):
            hit = at == p * step - step // 2
            out = hit if out is None else out | hit
        return out

    def images(self, plan, planes, source, k):
        values = [planes[source + m] for m in range(4)]
        to_right = self.turns(self.j + 1, plan.cols, plan.width)
        to_left = self.turns(self.j, plan.cols, plan.width)
        to_low = self.turns(self.i + 1, plan.rows, plan.height)
        to_top = self.turns(self.i, plan.rows, plan.height)

        def shifted(reader, turn, step, later):
            seen = [reader(value, k + m) for m, value in enumerate(values)]
            out = list(seen)
            for m in range(4):
                if bool(m & step) == later:
                    out[m] = jnp.where(turn, seen[m ^ step], seen[m])
                else:
                    out[m] = jnp.where(turn, 0.0, seen[m])
            return out

        right = shifted(self.right, to_right, 1, True)
        left = shifted(self.left, to_left, 1, False)
        low = shifted(self.low, to_low, 2, True)
        top = shifted(self.top, to_top, 2, False)
        return [
            planes[CO] * values[m]
            - planes[CO + 1] * right[m]
            - planes[CO + 2] * left[m]
            - planes[CO + 3] * low[m]
            - planes[CO + 4] * top[m]
            for m in range(4)
        ]


def windows(plan):
    rows, cols = plan.rows, plan.cols
    i, j = iota((rows, cols), 0), iota((rows, cols), 1)
    base_row = jnp.zeros((rows, cols), F32) + (lax.axis_index("row") * plan.lv - 1).astype(F32)
    base_col = jnp.zeros((rows, cols), F32) + (lax.axis_index("col") * plan.cw - 1).astype(F32)
    for p in range(1, plan.parts):
        base_row = base_row + jnp.where(i >= p * plan.height - plan.height // 2, 1.0, 0.0)
    for p in range(1, plan.cw + 1):
        base_col = base_col + jnp.where(j >= p * plan.width - plan.width // 2, 1.0, 0.0)
    return base_row, base_col


def hits_of(label, base_row, base_col):
    high = jnp.floor(label * (1.0 / REG))
    a, b = high - base_row, label - REG * high - base_col
    return [(a == m) & (b == n) for m in (0.0, 1.0) for n in (0.0, 1.0)]


def add_sums(plan, s_ref, h, part, acc):
    n, hn = plan.loads, plan.half
    for a in (0, 1):
        for b in (0, 1):
            at = (part + a) * n + h * hn
            s_ref[b, at : at + hn, :] = s_ref[b, at : at + hn, :] + acc[2 * a + b]


def packed(plan, s_ref):
    out = [None] * (plan.cw + 2)
    half = plan.width // 2
    for b in (0, 1):
        turned = s_ref[b].T
        for g in range(plan.cw + 1):
            part = turned[max(0, g * plan.width - half) : min(plan.cols, g * plan.width + half)]
            term = jnp.sum(part, axis=0, keepdims=True)
            out[g + b] = term if out[g + b] is None else out[g + b] + term
    out.append(jnp.zeros((8 - len(out), LANES), F32))
    return jnp.concatenate(out, axis=0)


def pair_sums(plan, planes, x, y, pair_ref, q):
    terms = {}
    for part, first, last in plan.chunks():
        for k in range(4):
            for m in range(4):
                da, db = m // 2 - k // 2, m % 2 - k % 2
                at = (k % 2, (part + k // 2) * BLOCK + q + (da + 1) * 3 + db + 1)
                term = jnp.sum(planes[x + k, first:last, :] * planes[y + m, first:last, :], axis=0, keepdims=True)
                terms[at] = term if at not in terms else terms[at] + term
    for (b, at), term in terms.items():
        pair_ref[b, at : at + 1, :] = term


class Spread:
    def __init__(self, plan, legs, planes, sides, got_planes, got_sides):
        self.plan, self.planes, self.sides = plan, planes, sides
        self.got_planes, self.got_sides = got_planes, got_sides
        west, east = sides.at[0], sides.at[1]
        self.legs = legs
        self.mine = legs.make([
            (1, 0, planes, got_planes.at[0]),
            (-1, 0, planes, got_planes.at[1]),
            (0, -1, west, got_sides.at[0]),
            (1, -1, west, got_sides.at[1]),
            (-1, -1, west, got_sides.at[2]),
            (0, 1, east, got_sides.at[3]),
            (1, 1, east, got_sides.at[4]),
            (-1, 1, east, got_sides.at[5]),
        ])

    def send(self, values):
        last = self.plan.cw + 1
        for k, value in enumerate(values):
            self.planes[k] = value
            self.sides[0, k : k + 1, :] = value[:1]
            self.sides[1, k : k + 1, :] = value[last : last + 1]
        self.legs.start(self.mine)

    def meet(self, own, above, below):
        lv = self.plan.lv
        block = iota(own.shape, len(own.shape) - 1) // BLOCK
        shift = lv * BLOCK
        return own + jnp.where(block == 1, rolled(above, -shift, 1), 0.0) + jnp.where(block == lv, rolled(below, shift, 1), 0.0)

    def merged(self):
        self.legs.wait(self.mine)
        sub = iota((8, LANES), 0)
        sides = self.got_sides
        right = self.meet(sides[0], sides[1], sides[2])
        left = self.meet(sides[3], sides[4], sides[5])
        out = []
        for k in range(self.planes.shape[0]):
            value = self.meet(self.planes[k], self.got_planes[0, k], self.got_planes[1, k])
            value = value + jnp.where(sub == self.plan.cw, right[k : k + 1], 0.0) + jnp.where(sub == 1, left[k : k + 1], 0.0)
            out.append(value)
        return out


def message(plan, pieces):
    sub, block = iota((8, LANES), 0), iota((8, LANES), 1) // BLOCK
    out = jnp.zeros((8, LANES), F32)
    for spot, value in pieces:
        for l in range(plan.lv):
            first = l * plan.cw
            moved = rolled(rolled(value, first - 1, 0), BLOCK * (spot - 1 - l), 1)
            out = jnp.where((block == spot) & (sub >= first) & (sub < first + plan.cw), moved, out)
    return out


def fold(value):
    half = value + pltpu.roll(value, 2 * BLOCK, 1)
    return half + pltpu.roll(half, BLOCK, 1)


def same(value, spot):
    return fold(jnp.where(iota(value.shape, 1) // BLOCK == spot, value, 0.0))


def dot(a, b, contract=((1,), (0,))):
    return lax.dot_general(a, b, (contract, ((), ())), precision=precise, preferred_element_type=F32)


def taken(value, index):
    return jnp.take_along_axis(value, index, axis=1, mode="promise_in_bounds")


def small_inverses(value):
    lane, sub = iota(value.shape, 1), iota(value.shape, 0)
    start = lane // REG * REG
    cols = [taken(value, start + j) for j in range(REG)]
    for k in range(REG):
        col = cols[k]
        here = sub == k
        recip = 1.0 / col[k : k + 1]
        left = jnp.where(here, -1.0, col)
        for j in range(REG):
            if j != k:
                row = cols[j][k : k + 1] * recip
                cols[j] = jnp.where(here, 0.0, cols[j]) - left * row
        cols[k] = jnp.where(here, recip, -col * recip)
    out = cols[0]
    for j in range(1, REG):
        out = jnp.where(lane % REG == j, cols[j], out)
    return out


def block_inverses(matrix, first, count):
    width = matrix.shape[1]
    lane, sub = iota((REG, width), 1), iota((REG, width), 0)
    value = jnp.where(lane % REG == sub, 1.0, 0.0)
    for q in range(first, first + count):
        value = jnp.where(lane // REG == q, matrix[q * REG : (q + 1) * REG], value)
    value = small_inverses(value)
    return jnp.concatenate([jnp.where(lane // REG == q, value, 0.0) for q in range(first, first + count)], axis=0)


def placed(value, first, total):
    pieces = []
    if first:
        pieces.append(jnp.zeros((first, value.shape[1]), F32))
    pieces.append(value)
    rest = total - first - value.shape[0]
    if rest:
        pieces.append(jnp.zeros((rest, value.shape[1]), F32))
    return jnp.concatenate(pieces, axis=0) if len(pieces) > 1 else value


def tail_inverse(matrix, first, count):
    size = matrix.shape[0]
    if count == 1:
        return block_inverses(matrix, first, 1)
    a, b, c = first * REG, (first + count // 2) * REG, (first + count) * REG
    lane = iota((1, size), 1)
    early, late = (lane >= a) & (lane < b), (lane >= b) & (lane < c)
    x = block_inverses(matrix, first, count // 2)
    f = placed(jnp.where(late, matrix[a:b], 0.0), a, size)
    y = dot(x, f)
    y_full = placed(y, a, size)
    rest = matrix[b:c] - dot(jnp.where(early, matrix[b:c], 0.0), y_full)
    rest = jnp.where(late, rest, 0.0)
    inner = tail_inverse(placed(rest, b, size), first + count // 2, count // 2)
    t = dot(y, placed(inner, b, size))
    top = jnp.where(early, x + dot(t, y_full, ((1,), (1,))), -t)
    turned = placed(t, a, size).T
    low = jnp.where(early, -turned[b:c], inner)
    return jnp.concatenate([top, low], axis=0)


def whole_inverse(matrix, between):
    half = matrix.shape[0] // 2
    x = block_inverses(matrix[:half, :half], 0, half // REG)
    y = dot(x, matrix[:half, half:])
    rest = matrix[half:, half:] - dot(matrix[half:, :half], y)
    inner = tail_inverse(rest, 0, half // REG)
    between()
    t = dot(y, inner)
    top = jnp.concatenate([x + dot(t, y, ((1,), (1,))), -t], axis=1)
    return jnp.concatenate([top, jnp.concatenate([-t.T, inner], axis=1)], axis=0)


def region_of(at):
    q = at // REG
    row = jnp.where(q < 8, 2 * q, jnp.where(q < 12, 4 * q - 31, jnp.where(q < 14, 8 * q - 93, jnp.where(q < 15, 7, 15))))
    return row * REG + at % REG


def coarse_matrix(value, first):
    size = value.shape[0]
    gap = region_of(iota((size, size), 1)) - region_of(iota((size, size), 0))
    total = jnp.zeros((size, size), F32)
    for k in range(9):
        total = jnp.where(gap == REG * (k // 3 - 1) + k % 3 - 1, value[:, first + k : first + k + 1], total)
    return total


def banded(diag_ref, pad_ref):
    out = []
    for q in range(REG):
        total = None
        for k in range(9):
            row = ORDER[q] + k // 3 - 1
            if 0 <= row < REG:
                at = 8 + REG * ORDER.index(row) + k % 3 - 1
                term = diag_ref[k, q * REG : (q + 1) * REG, :] * pad_ref[at : at + REG, :]
                total = term if total is None else total + term
        out.append(total)
    return jnp.concatenate(out, axis=0)


def wide(value):
    return jnp.broadcast_to(value, (LANES, LANES)).T[:BLOCK]


def front_kernel(
    plan, b_hbm, h_ref, v_ref, label_ref, bump_ref, pad_class_ref, edge_table, pad_table,
    b1_out, b2_out, planes_out, cx_ref, wide_ref,
    braw, bt, u0, u1, b1, b2, planes, ea, eb, ec, ga, gb, gc, brow, bcol, ccol, cpack, cpack1, hp,
    s0, s1, s2, s3, s4, pa, pb, pc, tacc,
    set0, set1, set2, side0, side1, side2, gset0, gset1, gset2, gside0, gside1, gside2,
    note, gat, q0, q1, q2, cpad, diag, knat,
    in_sem, out_sem, send_sem, recv_sem, note_send, note_recv,
):
    rows, cols, n, hn = plan.rows, plan.cols, plan.loads, plan.half
    r, c = lax.axis_index("row"), lax.axis_index("col")
    me = r * plan.nc + c
    count = plan.count
    barrier = pltpu.get_barrier_semaphore()

    def device(d):
        other = lax.rem(me + d, count)
        return (other // plan.nc, lax.rem(other, plan.nc))

    def fetch(k):
        return pltpu.make_async_copy(b_hbm.at[k], braw.at[pl.ds(pl.multiple_of(k * plan.pitch, 8), rows)], in_sem.at[k])

    def fetch_start(k, carry):
        fetch(k).start()
        return carry

    def fetch_wait(k, carry):
        fetch(k).wait()
        return carry

    lax.fori_loop(0, n, fetch_start, 0)
    for ref in (ga, gb, gc, brow, bcol, ccol, gset0, gset1, gset2, gside0, gside1, gside2):
        ref[...] = jnp.zeros_like(ref)
    u1[0:n, :] = jnp.zeros((n, cols), F32)
    u1[(rows + 1) * n :, :] = jnp.zeros((n, cols), F32)

    def greet(d, carry):
        pl.semaphore_signal(barrier, inc=1, device_id=device(d), device_id_type=pl.DeviceIdType.MESH)
        return carry

    lax.fori_loop(1, count, greet, 0)

    i, j = iota((rows, cols), 0), iota((rows, cols), 1)
    row_end = jnp.where(r == plan.nr - 1, rows - 1, rows)
    col_end = jnp.where(c == plan.nc - 1, cols - 1, cols)
    planes[CO + 1] = jnp.where(j == col_end, 0.0, looked_up(edge_table, h_ref[...]))
    planes[CO + 3] = jnp.where(i == row_end, 0.0, looked_up(edge_table, v_ref[...]))
    for ref in (ea, eb, ec):
        ref[...] = jnp.zeros_like(ref)
    put_edges(ea, 0, label_ref[...].astype(F32))
    put_edges(ea, 1, bump_ref[...])
    put_edges(ea, 2, planes[CO + 1])
    put_edges(ea, 3, planes[CO + 3])
    legs = Legs(plan, send_sem, recv_sem)
    first_edges = legs.make(beside(ea, ga))
    base_row, base_col = windows(plan)
    bump = bump_ref[...]
    for k, hit in enumerate(hits_of(label_ref[...].astype(F32), base_row, base_col)):
        planes[Z + k] = jnp.where(hit, bump, 0.0)
    pl.semaphore_wait(barrier, count - 1)
    legs.start(first_edges)

    for ref in (s0, s1, s2, s3, s4, pa, pb, pc):
        ref[...] = jnp.zeros_like(ref)
    lax.fori_loop(0, n, fetch_wait, 0)

    def packs(pack, value, k):
        left, right = pack
        lane = iota(value.shape, 1)
        moved = pltpu.roll(value, k, 1)
        return jnp.where(lane == k, moved, left), jnp.where(lane == lax.rem(k + cols - 1, cols), moved, right)

    zero = jnp.zeros((hn, cols), F32)
    for h in (0, 1):
        pack = (zero, zero)
        for part, first, last in plan.chunks():

            def step(k, u, carry):
                acc, pack = carry
                v = braw[pl.ds(k + h * hn * plan.pitch, hn, stride=plan.pitch), :]
                bt[pl.ds(pl.multiple_of(k * n + h * hn, 8), hn), :] = v
                return tuple(x + row_of(planes, Z + m, k) * v for m, x in enumerate(acc)), packs(pack, v, k)

            acc, pack = over_rows(first, last, step, ((zero,) * 4, pack))
            add_sums(plan, s0, h, part, acc)
        cpack[0, h * hn : (h + 1) * hn, :] = pack[1]
        cpack[1, h * hn : (h + 1) * hn, :] = pack[0]
    load_edges = legs.make([
        (1, 0, bt.at[pl.ds((rows - 1) * n, n)], brow.at[0]),
        (-1, 0, bt.at[pl.ds(0, n)], brow.at[1]),
        (0, 1, cpack.at[0], bcol.at[0]),
        (0, -1, cpack.at[1], bcol.at[1]),
    ])
    legs.start(load_edges)

    legs.wait(first_edges)
    around = Around(ga, rows, cols)
    right, down = planes[CO + 1], planes[CO + 3]
    left, upper = around.left(right, 2), around.top(down, 3)
    diagonal = looked_up(pad_table, pad_class_ref[...]) + right + left + down + upper
    minv = 1.0 / diagonal
    planes[CO] = diagonal
    planes[CO + 2] = left
    planes[CO + 4] = upper
    planes[MINV] = minv
    named = label_ref[...].astype(F32)
    bump = bump_ref[...]
    total = None
    for label, weight in (
        (named, diagonal * bump),
        (around.right(named, 0), -right * around.right(bump, 1)),
        (around.left(named, 0), -left * around.left(bump, 1)),
        (around.low(named, 0), -down * around.low(bump, 1)),
        (around.top(named, 0), -upper * around.top(bump, 1)),
    ):
        terms = [jnp.where(hit, weight, 0.0) for hit in hits_of(label, base_row, base_col)]
        total = terms if total is None else [t + u for t, u in zip(total, terms)]
    put_edges(eb, 0, minv)
    for k in range(4):
        planes[W0 + k] = total[k]
        value = total[k] * minv
        planes[V0 + k] = value
        put_edges(eb, 1 + k, value)
    image_edges = legs.make(beside(eb, gb))
    legs.start(image_edges)

    pair_sums(plan, planes, Z, W0, pa, 0)
    spread0 = Spread(plan, legs, set0, side0, gset0, gside0)
    spread0.send([packed(plan, s0), packed(plan, pa)])

    for h in (0, 1):
        dots = zero
        for part, first, last in plan.chunks():

            def step(k, u, carry):
                dots, acc = carry
                v = bt[pl.ds(pl.multiple_of(k * n + h * hn, 8), hn), :]
                w = row_of(planes, MINV, k) * v
                u0[pl.ds(pl.multiple_of((k + 1) * n + h * hn, 8), hn), :] = w
                return dots + v * w, tuple(x + row_of(planes, V0 + m, k) * v for m, x in enumerate(acc))

            dots, acc = over_rows(first, last, step, (dots, (zero,) * 4))
            add_sums(plan, s1, h, part, acc)
        tacc[h * hn : (h + 1) * hn, :] = dots

    def note_copy(m, d):
        return pltpu.make_async_remote_copy(
            src_ref=note.at[m],
            dst_ref=gat.at[m, me],
            send_sem=note_send.at[m, d],
            recv_sem=note_recv.at[m, d],
            device_id=device(d),
            device_id_type=pl.DeviceIdType.MESH,
        )

    def tell(m, value):
        note[m] = value
        gat[m, pl.ds(me, 1)] = value[None]

        def go(d, carry):
            note_copy(m, d).start()
            return carry

        lax.fori_loop(1, count, go, 0)

    def hear(m):
        def go(d, carry):
            note_copy(m, d).wait()
            return carry

        lax.fori_loop(1, count, go, 0)

    load_sums, energy = spread0.merged()
    tell(0, message(plan, [(0, load_sums), (1, energy)]))

    def halo_columns(from_left, from_right):
        even = iota((n, cols), 1) % 2 == 0
        from_right = pltpu.roll(from_right, cols - 1, 1)
        hp[0] = jnp.where(even, from_left, from_right)
        hp[1] = jnp.where(even, from_right, from_left)

    legs.wait(load_edges)
    legs.wait(image_edges)
    u0[0:n, :] = brow[0] * gb[0, 0:1, :]
    u0[(rows + 1) * n :, :] = brow[1] * gb[1, 0:1, :]
    halo_columns(pltpu.roll(bcol[0], 1, 1) * gb[2, 0:1, :], bcol[1] * gb[3, 0:1, :])
    around = Around(gb, rows, cols)
    for k, value in enumerate(around.images(plan, planes, V0, 1)):
        planes[W1 + k] = value
        value = value * planes[MINV]
        planes[V1 + k] = value
        put_edges(ec, k, value)
    next_edges = legs.make(beside(ec, gc))
    legs.start(next_edges)

    lane = iota((hn, cols), 1)

    def stencil(field, h, k, u):
        def at(t):
            return field[pl.ds(pl.multiple_of(t * n + h * hn, 8), hn), :]

        z = at(k + 1)
        halo = pltpu.roll(hp[u % 2, h * hn : (h + 1) * hn, :], lax.rem(cols - k, cols), 1)
        before = jnp.where(lane == 0, halo, pltpu.roll(z, 1, 1))
        after = jnp.where(lane == cols - 1, halo, pltpu.roll(z, cols - 1, 1))
        f = (
            row_of(planes, CO, k) * z
            - row_of(planes, CO + 1, k) * after
            - row_of(planes, CO + 2, k) * before
            - row_of(planes, CO + 3, k) * at(k + 2)
            - row_of(planes, CO + 4, k) * at(k)
        )
        return z, f

    for h in (0, 1):
        pack, dots, more = (zero, zero), zero, zero
        for part, first, last in plan.chunks():

            def step(k, u, carry):
                dots, more, acc, bcc, pack = carry
                z, f = stencil(u0, h, k, u)
                w = row_of(planes, MINV, k) * f
                b1[pl.ds(pl.multiple_of(k * n + h * hn, 8), hn), :] = f
                u1[pl.ds(pl.multiple_of((k + 1) * n + h * hn, 8), hn), :] = w
                acc = tuple(x + row_of(planes, V0 + m, k) * f for m, x in enumerate(acc))
                bcc = tuple(x + row_of(planes, V1 + m, k) * f for m, x in enumerate(bcc))
                return dots + z * f, more + w * f, acc, bcc, packs(pack, w, k)

            dots, more, acc, bcc, pack = over_rows(first, last, step, (dots, more, (zero,) * 4, (zero,) * 4, pack))
            add_sums(plan, s2, h, part, acc)
            add_sums(plan, s3, h, part, bcc)
        tacc[n + h * hn : n + (h + 1) * hn, :] = dots
        tacc[2 * n + h * hn : 2 * n + (h + 1) * hn, :] = more
        cpack1[0, h * hn : (h + 1) * hn, :] = pack[1]
        cpack1[1, h * hn : (h + 1) * hn, :] = pack[0]
    field_edges = legs.make([
        (1, 0, u1.at[pl.ds(rows * n, n)], u1.at[pl.ds(0, n)]),
        (-1, 0, u1.at[pl.ds(n, n)], u1.at[pl.ds((rows + 1) * n, n)]),
        (0, 1, cpack1.at[0], ccol.at[0]),
        (0, -1, cpack1.at[1], ccol.at[1]),
    ])
    legs.start(field_edges)
    out1 = pltpu.make_async_copy(b1, b1_out, out_sem.at[0])
    out1.start()

    pair_sums(plan, planes, W0, V0, pb, 0)
    pair_sums(plan, planes, W1, V0, pb, 9)
    pair_sums(plan, planes, W1, V1, pb, 18)
    spread1 = Spread(plan, legs, set1, side1, gset1, gside1)
    spread1.send([packed(plan, s1), packed(plan, s2), packed(plan, s3), packed(plan, pb)])

    legs.wait(next_edges)
    around = Around(gc, rows, cols)
    for k, value in enumerate(around.images(plan, planes, V1, 0)):
        planes[W2 + k] = value
    out0 = pltpu.make_async_copy(planes.at[pl.ds(0, KEPT)], planes_out, out_sem.at[1])
    out0.start()
    legs.wait(field_edges)
    halo_columns(pltpu.roll(ccol[0], 1, 1), ccol[1])

    for h in (0, 1):
        dots = zero
        for part, first, last in plan.chunks():

            def step(k, u, carry):
                dots, acc = carry
                z, f = stencil(u1, h, k, u)
                b2[pl.ds(pl.multiple_of(k * n + h * hn, 8), hn), :] = f
                return dots + z * f, tuple(x + row_of(planes, V1 + m, k) * f for m, x in enumerate(acc))

            dots, acc = over_rows(first, last, step, (dots, (zero,) * 4))
            add_sums(plan, s4, h, part, acc)
        tacc[3 * n + h * hn : 3 * n + (h + 1) * hn, :] = dots
    out2 = pltpu.make_async_copy(b2, b2_out, out_sem.at[2])
    out2.start()
    pair_sums(plan, planes, W2, V1, pc, 0)
    spread2 = Spread(plan, legs, set2, side2, gset2, gside2)
    spread2.send([packed(plan, pc), packed(plan, s4)])
    dots = jnp.sum(tacc[...].T, axis=0, keepdims=True)

    first_sums, second_sums, third_sums, pairs = spread1.merged()
    tell(1, message(plan, [(0, first_sums), (1, second_sums), (2, third_sums), (3, pairs)]))

    def settle(m, ref):
        hear(m)
        for d in range(count):
            for l in range(plan.lv):
                at = REG * ORDER.index(d // plan.nc * plan.lv + l) + d % plan.nc * plan.cw
                ref[at : at + plan.cw, :] = gat[m, d, l * plan.cw : (l + 1) * plan.cw, :]

    def last_message():
        last_pairs, last_sums = spread2.merged()
        value = message(plan, [(0, last_pairs), (3, last_sums)])
        sub, block = iota((8, LANES), 0), iota((8, LANES), 1) // BLOCK
        for k in range(4):
            value = jnp.where((sub == k) & (block == 1), rolled(dots, BLOCK * (1 - k), 1), value)
        tell(2, value)

    settle(0, q0)
    inverse = whole_inverse(coarse_matrix(q0[...], BLOCK), last_message)
    c0 = same(dot(inverse, q0[...]), 0)
    settle(1, q1)
    settle(2, q2)

    regions = c0.shape[0]
    block = iota((regions, LANES), 1) // BLOCK
    pair_values = jnp.where(block == 3, q1[...], q2[...])
    sums = jnp.where(block == 3, q2[...], q1[...])
    start = jnp.where(block == 3, 0, 3 * BLOCK + 9 * block)
    for k in range(9):
        diag[k] = taken(pair_values, start + k)
    all_dots = jnp.sum(gat[2], axis=0)
    row_block = iota((1, LANES), 1) // BLOCK
    dots = jnp.zeros((1, LANES), F32)
    for k in range(4):
        dots = jnp.where(row_block == k, rolled(all_dots[k : k + 1], BLOCK * (k - 1), 1), dots)

    def over(value):
        return jnp.sum(value, axis=0, keepdims=True)

    cpad[...] = jnp.zeros_like(cpad)
    cpad[8 : 8 + regions, :] = c0
    reduced = sums - banded(diag, cpad)
    dots = dots - over(c0 * (sums + reduced))
    rho, m1, m2, m3 = [same(dots, k) for k in range(4)]
    solved = dot(inverse, reduced)
    c1, e2 = same(solved, 0), same(solved, 1)
    cpad[8 : 8 + regions, :] = c1
    image = banded(diag, cpad)
    in_c1 = over(c1 * reduced)
    image_c1 = over(c1 * image)
    with_s1, with_s2, with_s3 = [same(in_c1, k) for k in range(3)]
    curve = m1 - with_s1
    alpha = rho / curve
    square = m2 - 2.0 * with_s2 + same(image_c1, 0)
    turned = same(dot(inverse, image), 0)
    c2 = c1 - alpha * (e2 - turned)
    now = reduced - alpha * (pltpu.roll(reduced, 3 * BLOCK, 1) - image)
    in_c2 = same(over(c2 * now), 0)
    image_dot = m1 - 2.0 * alpha * (m2 - with_s2) + alpha * alpha * (m3 - 2.0 * with_s3 + same(image_c1, 1))
    rho1 = rho - 2.0 * alpha * curve + alpha * alpha * square
    beta = rho1 / rho
    curve1 = image_dot - in_c2 + 2.0 * beta * (curve - alpha * square) + beta * beta * curve
    alpha1 = rho1 / curve1
    mix = alpha + alpha1 * beta
    kappa, lam = mix + alpha1, alpha * alpha1
    coefs = jnp.where(block == 0, c0 - mix * c1 - alpha1 * c2, jnp.where(block == 1, lam * c1 - kappa * c0, lam * c0))
    wide_ref[0] = wide(kappa)
    wide_ref[1] = wide(lam)

    knat[...] = jnp.zeros_like(knat)
    for q in range(REG):
        at = REG * (1 + ORDER[q])
        knat[at : at + REG, :] = coefs[q * REG : (q + 1) * REG]
    near = knat[pl.ds(pl.multiple_of(r * (plan.lv * REG), REG), LANES), :].T
    base = c * plan.cw - 1 + (iota((3 * BLOCK, cols), 1) + plan.width // 2) // plan.width
    for b in (0, 1):
        column = jnp.clip(base + b, 0, REG - 1)
        for l in range(plan.levels):
            value = taken(near[: 3 * BLOCK], column + l * REG)
            for f in range(3):
                cx_ref[f, b, l * n : (l + 1) * n, :] = value[f * BLOCK : f * BLOCK + n]

    out0.wait()
    out1.wait()
    out2.wait()
    legs.finish()


def last_kernel(
    plan, b_hbm, b1_hbm, b2_hbm, planes_hbm, cx_ref, wide_ref, x_hbm, r_hbm,
    braw, b1, b2, planes, xs, rs, in_sem, out_sem,
):
    n, hn = plan.loads, plan.half
    flat_b = braw.reshape(n * plan.pitch, plan.cols)
    flat_x = xs.reshape(n * plan.pitch, plan.cols)
    flat_r = rs.reshape(n * plan.pitch, plan.cols)
    arrivals, departures = [], []
    for part, first, last in plan.chunks():
        here, flat = pl.ds(first, last - first), pl.ds(first * n, (last - first) * n)
        arrivals.append([
            pltpu.make_async_copy(src, dst, in_sem.at[part, k])
            for k, (src, dst) in enumerate((
                (planes_hbm.at[:, here], planes.at[:, here]),
                (b_hbm.at[:, here], braw.at[:, here]),
                (b1_hbm.at[flat], b1.at[flat]),
                (b2_hbm.at[flat], b2.at[flat]),
            ))
        ])
        departures.append([
            pltpu.make_async_copy(xs.at[:, here], x_hbm.at[:, here], out_sem.at[part, 0]),
            pltpu.make_async_copy(rs.at[:, here], r_hbm.at[:, here], out_sem.at[part, 1]),
        ])
    for copies in arrivals:
        for copy in copies:
            copy.start()
    for part, first, last in plan.chunks():
        for copy in arrivals[part]:
            copy.wait()
        for h in (0, 1):
            kappa, lam = [wide_ref[k, h * hn : (h + 1) * hn, :] for k in (0, 1)]
            cx = []
            for f in range(3):
                for a in (0, 1):
                    for b in (0, 1):
                        at = (part + a) * n + h * hn
                        cx.append(cx_ref[f, b, at : at + hn, :])

            def step(k, u, carry):
                at = pl.ds(pl.multiple_of(k * n + h * hn, 8), hn)
                to = pl.ds(k + h * hn * plan.pitch, hn, stride=plan.pitch)
                v0, v1, v2 = flat_b[to, :], b1[at, :], b2[at, :]
                x = kappa * v0 - lam * v1
                r = v0 - kappa * v1 + lam * v2
                plain = None
                for m in range(4):
                    w0 = row_of(planes, W0 + m, k)
                    w1 = row_of(planes, W1 + m, k)
                    x = x + w0 * cx[4 + m] + w1 * cx[8 + m]
                    r = r - w0 * cx[m] - w1 * cx[4 + m] - row_of(planes, W2 + m, k) * cx[8 + m]
                    term = row_of(planes, Z + m, k) * cx[m]
                    plain = term if plain is None else plain + term
                flat_x[to, :] = row_of(planes, MINV, k) * x + plain
                flat_r[to, :] = r
                return carry

            over_rows(first, last, step, 0, 4)
        for copy in departures[part]:
            copy.start()
    for copies in departures:
        for copy in copies:
            copy.wait()


def body(load_currents, labels, bump_height, horizontal_class, vertical_class, pad_class, edge_table, pad_table):
    rows, cols = labels.shape
    loads = load_currents.shape[0]
    nr, nc = lax.axis_size("row"), lax.axis_size("col")
    height, width = nr * rows // REG, nc * cols // REG
    plan = Plan(rows, cols, loads, height, width, nr, nc)
    n, regions, count = loads, REG * REG, plan.count
    field = (rows * n, cols)
    tall = ((rows + 2) * n, cols)
    edge = (4, 8, cols)
    sums = (2, LANES, cols)

    def vm(*dims):
        return pltpu.VMEM(dims, F32)

    def dma(*dims):
        return pltpu.SemaphoreType.DMA(dims)

    legs = 4 * 5 + 3 * 8
    b1, b2, planes, cx, scales = pl.pallas_call(
        functools.partial(front_kernel, plan),
        out_shape=(shape(*field), shape(*field), shape(KEPT, rows, cols), shape(3, 2, plan.levels * n, cols), shape(2, n, cols)),
        in_specs=[ANY] + [VM] * 5 + [SM] * 2,
        out_specs=(ANY, ANY, ANY, VM, VM),
        scratch_shapes=[
            vm(n * plan.pitch, cols), vm(*field), vm(*tall), vm(*tall), vm(*field), vm(*field), vm(PLANES, rows, cols),
            vm(*edge), vm(*edge), vm(*edge), vm(*edge), vm(*edge), vm(*edge),
            vm(2, n, cols), vm(2, n, cols), vm(2, n, cols), vm(2, n, cols), vm(2, n, cols), vm(2, n, cols),
        ] + [vm(*sums)] * 8 + [
            vm(LANES, LANES),
            vm(2, 8, LANES), vm(4, 8, LANES), vm(2, 8, LANES), vm(2, 8, LANES), vm(2, 8, LANES), vm(2, 8, LANES),
            vm(2, 2, 8, LANES), vm(2, 4, 8, LANES), vm(2, 2, 8, LANES), vm(6, 8, LANES), vm(6, 8, LANES), vm(6, 8, LANES),
            vm(3, 8, LANES), vm(3, count, 8, LANES), vm(regions, LANES), vm(regions, LANES), vm(regions, LANES),
            vm(regions + 16, LANES), vm(9, regions, LANES), vm(regions + LANES + 2 * REG, LANES),
            dma(n), dma(3), dma(legs), dma(legs), dma(3, count), dma(3, count),
        ],
        compiler_params=pltpu.CompilerParams(collective_id=0, has_side_effects=True, vmem_limit_bytes=56 * 1024 * 1024),
    )(load_currents, horizontal_class, vertical_class, labels, bump_height, pad_class, edge_table, pad_table)
    staged = (n, plan.pitch, cols)
    return pl.pallas_call(
        functools.partial(last_kernel, plan),
        out_shape=(shape(n, rows, cols),) * 2,
        in_specs=[ANY] * 4 + [VM] * 2,
        out_specs=(ANY, ANY),
        scratch_shapes=[
            vm(*staged), vm(*field), vm(*field), vm(KEPT, rows, cols), vm(*staged), vm(*staged),
            dma(plan.parts, 4), dma(plan.parts, 2),
        ],
        compiler_params=pltpu.CompilerParams(vmem_limit_bytes=56 * 1024 * 1024),
    )(load_currents, b1, b2, planes, cx, scales)


def solution(mesh):
    grid = P("row", "col")
    cube = P(None, "row", "col")
    return jax.shard_map(
        body,
        mesh=mesh,
        in_specs=(cube, grid, grid, grid, grid, grid, P(), P()),
        out_specs=(cube, cube),
        check_vma=False,
    )
```

```python
import functools

import jax
import jax.numpy as jnp
from jax import lax
from jax.experimental import pallas as pl
from jax.experimental.pallas import tpu as pltpu
from jax.sharding import PartitionSpec as P

REG = 16
F32 = jnp.float32
precise = lax.Precision.HIGHEST
VM = pl.BlockSpec(memory_space=pltpu.VMEM)
SM = pl.BlockSpec(memory_space=pltpu.SMEM)
ANY = pl.BlockSpec(memory_space=pl.ANY)
BLOCK = 32
LANES = 4 * BLOCK
PITCH = 8
GROUP = 32
MINV, Z, W0, W1, W2, V0, V1, CO = 0, 1, 5, 9, 13, 17, 21, 25
KEPT, PLANES = 17, 32
RIGHT_IN, LEFT_IN = 30, 31
ORDER = (0, 2, 4, 6, 8, 10, 12, 14, 1, 5, 9, 13, 3, 11, 7, 15)


def shape(*dims):
    return jax.ShapeDtypeStruct(dims, F32)


def iota(dims, axis):
    return lax.broadcasted_iota(jnp.int32, dims, axis)


def rolled(value, shift, axis):
    shift = shift % value.shape[axis]
    return pltpu.roll(value, shift, axis) if shift else value


class Plan:
    def __init__(self, rows, cols, loads, height, width, row_devices, col_devices):
        self.rows, self.cols, self.loads = rows, cols, loads
        self.height, self.width = height, width
        self.nr, self.nc = row_devices, col_devices
        self.count = row_devices * col_devices
        self.lv, self.cw = rows // height, cols // width
        self.parts = self.lv + 1
        self.levels = self.lv + 2
        self.half = loads // 2
        self.pitch = rows + PITCH

    def chunks(self):
        half = self.height // 2
        for part in range(self.parts):
            yield part, max(0, part * self.height - half), min(self.rows, part * self.height + half)


def over_rows(first, last, step, init, group=4):
    def body(g, carry):
        for u in range(group):
            carry = step(first + g * group + u, u, carry)
        return carry

    return lax.fori_loop(0, (last - first) // group, body, init)


def over_groups(first, last, group, init, size=8):
    return lax.fori_loop(0, (last - first) // size, lambda g, carry: group(first + g * size, carry), init)


def row_of(ref, k, i):
    return ref[k, pl.ds(i, 1), :]


class Legs:
    def __init__(self, plan, send_sem, recv_sem):
        self.plan, self.send_sem, self.recv_sem = plan, send_sem, recv_sem
        self.used = 0
        self.r, self.c = lax.axis_index("row"), lax.axis_index("col")
        self.everything = []

    def inside(self, dr, dc):
        r, c = self.r + dr, self.c + dc
        return (r >= 0) & (r < self.plan.nr) & (c >= 0) & (c < self.plan.nc)

    def make(self, items):
        out = []
        for dr, dc, src, dst in items:
            target = (lax.rem(self.r + dr + self.plan.nr, self.plan.nr), lax.rem(self.c + dc + self.plan.nc, self.plan.nc))
            copy = pltpu.make_async_remote_copy(
                src_ref=src,
                dst_ref=dst,
                send_sem=self.send_sem.at[self.used],
                recv_sem=self.recv_sem.at[self.used],
                device_id=target,
                device_id_type=pl.DeviceIdType.MESH,
            )
            self.used += 1
            out.append((self.inside(dr, dc), self.inside(-dr, -dc), copy))
        self.everything += out
        return out

    def start(self, legs):
        for goes, _, copy in legs:
            pl.when(goes)(copy.start)

    def wait(self, legs):
        for _, comes, copy in legs:
            pl.when(comes)(copy.wait_recv)

    def finish(self):
        for goes, _, copy in self.everything:
            pl.when(goes)(copy.wait_send)


def beside(src, dst):
    return [(1, 0, src.at[0], dst.at[0]), (-1, 0, src.at[1], dst.at[1]), (0, 1, src.at[2], dst.at[2]), (0, -1, src.at[3], dst.at[3])]


def looked_up(table_ref, classes):
    out = jnp.zeros(classes.shape, F32)
    for k in range(table_ref.shape[0]):
        out = jnp.where(classes == k, table_ref[k], out)
    return out


def put_edges(ref, k, value, row_end=True):
    rows, cols = value.shape
    ref[0, k : k + 1, :] = value[rows - 1 :]
    ref[1, k : k + 1, :] = value[:1]
    turned = value.T
    ref[2, k : k + 1, :] = turned[cols - 1 :]
    ref[3, k : k + 1, :] = turned[:1]


class Around:
    def __init__(self, edge_ref, rows, cols):
        self.edge_ref, self.rows, self.cols = edge_ref, rows, cols
        self.i, self.j = iota((rows, cols), 0), iota((rows, cols), 1)

    def column(self, side, k):
        return jnp.broadcast_to(self.edge_ref[side, k : k + 1, :], (self.cols, self.rows)).T

    def left(self, value, k):
        return jnp.where(self.j == 0, self.column(2, k), pltpu.roll(value, 1, 1))

    def right(self, value, k):
        return jnp.where(self.j == self.cols - 1, self.column(3, k), pltpu.roll(value, self.cols - 1, 1))

    def top(self, value, k):
        return jnp.where(self.i == 0, self.edge_ref[0, k : k + 1, :], pltpu.roll(value, 1, 0))

    def low(self, value, k):
        return jnp.where(self.i == self.rows - 1, self.edge_ref[1, k : k + 1, :], pltpu.roll(value, self.rows - 1, 0))

    def turns(self, at, size, step):
        out = None
        for p in range(1, size // step + 1):
            hit = at == p * step - step // 2
            out = hit if out is None else out | hit
        return out

    def images(self, plan, planes, source, k):
        values = [planes[source + m] for m in range(4)]
        to_right = self.turns(self.j + 1, plan.cols, plan.width)
        to_left = self.turns(self.j, plan.cols, plan.width)
        to_low = self.turns(self.i + 1, plan.rows, plan.height)
        to_top = self.turns(self.i, plan.rows, plan.height)

        def shifted(reader, turn, step, later):
            seen = [reader(value, k + m) for m, value in enumerate(values)]
            out = list(seen)
            for m in range(4):
                if bool(m & step) == later:
                    out[m] = jnp.where(turn, seen[m ^ step], seen[m])
                else:
                    out[m] = jnp.where(turn, 0.0, seen[m])
            return out

        right = shifted(self.right, to_right, 1, True)
        left = shifted(self.left, to_left, 1, False)
        low = shifted(self.low, to_low, 2, True)
        top = shifted(self.top, to_top, 2, False)
        return [
            planes[CO] * values[m]
            - planes[CO + 1] * right[m]
            - planes[CO + 2] * left[m]
            - planes[CO + 3] * low[m]
            - planes[CO + 4] * top[m]
            for m in range(4)
        ]


def windows(plan):
    rows, cols = plan.rows, plan.cols
    i, j = iota((rows, cols), 0), iota((rows, cols), 1)
    base_row = jnp.zeros((rows, cols), F32) + (lax.axis_index("row") * plan.lv - 1).astype(F32)
    base_col = jnp.zeros((rows, cols), F32) + (lax.axis_index("col") * plan.cw - 1).astype(F32)
    for p in range(1, plan.parts):
        base_row = base_row + jnp.where(i >= p * plan.height - plan.height // 2, 1.0, 0.0)
    for p in range(1, plan.cw + 1):
        base_col = base_col + jnp.where(j >= p * plan.width - plan.width // 2, 1.0, 0.0)
    return base_row, base_col


def hits_of(label, base_row, base_col):
    high = jnp.floor(label * (1.0 / REG))
    a, b = high - base_row, label - REG * high - base_col
    return [(a == m) & (b == n) for m in (0.0, 1.0) for n in (0.0, 1.0)]


def add_sums(plan, s_ref, h, part, acc):
    n, hn = plan.loads, plan.half
    for a in (0, 1):
        for b in (0, 1):
            at = (part + a) * n + h * hn
            s_ref[b, at : at + hn, :] = s_ref[b, at : at + hn, :] + acc[2 * a + b]


def packed(plan, s_ref):
    out = [None] * (plan.cw + 2)
    half = plan.width // 2
    for b in (0, 1):
        turned = s_ref[b].T
        for g in range(plan.cw + 1):
            part = turned[max(0, g * plan.width - half) : min(plan.cols, g * plan.width + half)]
            term = jnp.sum(part, axis=0, keepdims=True)
            out[g + b] = term if out[g + b] is None else out[g + b] + term
    out.append(jnp.zeros((8 - len(out), LANES), F32))
    return jnp.concatenate(out, axis=0)


def pair_sums(plan, planes, x, y, pair_ref, q):
    terms = {}
    for part, first, last in plan.chunks():
        for k in range(4):
            for m in range(4):
                da, db = m // 2 - k // 2, m % 2 - k % 2
                at = (k % 2, (part + k // 2) * BLOCK + q + (da + 1) * 3 + db + 1)
                term = jnp.sum(planes[x + k, first:last, :] * planes[y + m, first:last, :], axis=0, keepdims=True)
                terms[at] = term if at not in terms else terms[at] + term
    for (b, at), term in terms.items():
        pair_ref[b, at : at + 1, :] = term


class Spread:
    def __init__(self, plan, legs, planes, sides, got_planes, got_sides):
        self.plan, self.planes, self.sides = plan, planes, sides
        self.got_planes, self.got_sides = got_planes, got_sides
        west, east = sides.at[0], sides.at[1]
        self.legs = legs
        self.mine = legs.make([
            (1, 0, planes, got_planes.at[0]),
            (-1, 0, planes, got_planes.at[1]),
            (0, -1, west, got_sides.at[0]),
            (1, -1, west, got_sides.at[1]),
            (-1, -1, west, got_sides.at[2]),
            (0, 1, east, got_sides.at[3]),
            (1, 1, east, got_sides.at[4]),
            (-1, 1, east, got_sides.at[5]),
        ])

    def send(self, values):
        last = self.plan.cw + 1
        for k, value in enumerate(values):
            self.planes[k] = value
            self.sides[0, k : k + 1, :] = value[:1]
            self.sides[1, k : k + 1, :] = value[last : last + 1]
        self.legs.start(self.mine)

    def meet(self, own, above, below):
        lv = self.plan.lv
        block = iota(own.shape, len(own.shape) - 1) // BLOCK
        shift = lv * BLOCK
        return own + jnp.where(block == 1, rolled(above, -shift, 1), 0.0) + jnp.where(block == lv, rolled(below, shift, 1), 0.0)

    def merged(self):
        self.legs.wait(self.mine)
        sub = iota((8, LANES), 0)
        sides = self.got_sides
        right = self.meet(sides[0], sides[1], sides[2])
        left = self.meet(sides[3], sides[4], sides[5])
        out = []
        for k in range(self.planes.shape[0]):
            value = self.meet(self.planes[k], self.got_planes[0, k], self.got_planes[1, k])
            value = value + jnp.where(sub == self.plan.cw, right[k : k + 1], 0.0) + jnp.where(sub == 1, left[k : k + 1], 0.0)
            out.append(value)
        return out


def message(plan, pieces):
    sub, block = iota((8, LANES), 0), iota((8, LANES), 1) // BLOCK
    out = jnp.zeros((8, LANES), F32)
    for spot, value in pieces:
        for l in range(plan.lv):
            first = l * plan.cw
            moved = rolled(rolled(value, first - 1, 0), BLOCK * (spot - 1 - l), 1)
            out = jnp.where((block == spot) & (sub >= first) & (sub < first + plan.cw), moved, out)
    return out


def fold(value):
    half = value + pltpu.roll(value, 2 * BLOCK, 1)
    return half + pltpu.roll(half, BLOCK, 1)


def same(value, spot):
    return fold(jnp.where(iota(value.shape, 1) // BLOCK == spot, value, 0.0))


def dot(a, b, contract=((1,), (0,))):
    return lax.dot_general(a, b, (contract, ((), ())), precision=precise, preferred_element_type=F32)


def taken(value, index):
    return jnp.take_along_axis(value, index, axis=1, mode="promise_in_bounds")


def small_inverses(value):
    lane, sub = iota(value.shape, 1), iota(value.shape, 0)
    start = lane // REG * REG
    cols = [taken(value, start + j) for j in range(REG)]
    for k in range(REG):
        col = cols[k]
        here = sub == k
        recip = 1.0 / col[k : k + 1]
        left = jnp.where(here, -1.0, col)
        for j in range(REG):
            if j != k:
                row = cols[j][k : k + 1] * recip
                cols[j] = jnp.where(here, 0.0, cols[j]) - left * row
        cols[k] = jnp.where(here, recip, -col * recip)
    out = cols[0]
    for j in range(1, REG):
        out = jnp.where(lane % REG == j, cols[j], out)
    return out


def block_inverses(matrix, first, count):
    width = matrix.shape[1]
    lane, sub = iota((REG, width), 1), iota((REG, width), 0)
    value = jnp.where(lane % REG == sub, 1.0, 0.0)
    for q in range(first, first + count):
        value = jnp.where(lane // REG == q, matrix[q * REG : (q + 1) * REG], value)
    value = small_inverses(value)
    return jnp.concatenate([jnp.where(lane // REG == q, value, 0.0) for q in range(first, first + count)], axis=0)


def placed(value, first, total):
    pieces = []
    if first:
        pieces.append(jnp.zeros((first, value.shape[1]), F32))
    pieces.append(value)
    rest = total - first - value.shape[0]
    if rest:
        pieces.append(jnp.zeros((rest, value.shape[1]), F32))
    return jnp.concatenate(pieces, axis=0) if len(pieces) > 1 else value


def tail_inverse(matrix, first, count):
    size = matrix.shape[0]
    if count == 1:
        return block_inverses(matrix, first, 1)
    a, b, c = first * REG, (first + count // 2) * REG, (first + count) * REG
    lane = iota((1, size), 1)
    early, late = (lane >= a) & (lane < b), (lane >= b) & (lane < c)
    x = block_inverses(matrix, first, count // 2)
    f = placed(jnp.where(late, matrix[a:b], 0.0), a, size)
    y = dot(x, f)
    y_full = placed(y, a, size)
    rest = matrix[b:c] - dot(jnp.where(early, matrix[b:c], 0.0), y_full)
    rest = jnp.where(late, rest, 0.0)
    inner = tail_inverse(placed(rest, b, size), first + count // 2, count // 2)
    t = dot(y, placed(inner, b, size))
    top = jnp.where(early, x + dot(t, y_full, ((1,), (1,))), -t)
    turned = placed(t, a, size).T
    low = jnp.where(early, -turned[b:c], inner)
    return jnp.concatenate([top, low], axis=0)


def whole_inverse(matrix, between):
    half = matrix.shape[0] // 2
    x = block_inverses(matrix[:half, :half], 0, half // REG)
    y = dot(x, matrix[:half, half:])
    rest = matrix[half:, half:] - dot(matrix[half:, :half], y)
    between()
    inner = tail_inverse(rest, 0, half // REG)
    t = dot(y, inner)
    top = jnp.concatenate([x + dot(t, y, ((1,), (1,))), -t], axis=1)
    return jnp.concatenate([top, jnp.concatenate([-t.T, inner], axis=1)], axis=0)


def region_of(at):
    q = at // REG
    row = jnp.where(q < 8, 2 * q, jnp.where(q < 12, 4 * q - 31, jnp.where(q < 14, 8 * q - 93, jnp.where(q < 15, 7, 15))))
    return row * REG + at % REG


def coarse_matrix(value, first):
    size = value.shape[0]
    gap = region_of(iota((size, size), 1)) - region_of(iota((size, size), 0))
    total = jnp.zeros((size, size), F32)
    for k in range(9):
        total = jnp.where(gap == REG * (k // 3 - 1) + k % 3 - 1, value[:, first + k : first + k + 1], total)
    return total


def banded(diag_ref, pad_ref):
    out = []
    for q in range(REG):
        total = None
        for k in range(9):
            row = ORDER[q] + k // 3 - 1
            if 0 <= row < REG:
                at = 8 + REG * ORDER.index(row) + k % 3 - 1
                term = diag_ref[k, q * REG : (q + 1) * REG, :] * pad_ref[at : at + REG, :]
                total = term if total is None else total + term
        out.append(total)
    return jnp.concatenate(out, axis=0)


def wide(value):
    return jnp.broadcast_to(value, (LANES, LANES)).T[:BLOCK]


def front_kernel(
    plan, b_hbm, h_ref, v_ref, label_ref, bump_ref, pad_class_ref, edge_table, pad_table,
    b1_out, b2_out, planes_out, cx_ref, wide_ref,
    braw, bt, u0, u1, b1, b2, planes, ea, eb, ec, ga, gb, gc, brow, bcol, ccol, cpack, cpack1, beyond,
    s0, s1, s2, s3, s4, pa, pb, pc, tacc,
    set0, set1, set2, side0, side1, side2, gset0, gset1, gset2, gside0, gside1, gside2,
    note, gat, q0, q1, q2, cpad, diag, knat,
    in_sem, out_sem, send_sem, recv_sem, note_send, note_recv,
):
    rows, cols, n, hn = plan.rows, plan.cols, plan.loads, plan.half
    r, c = lax.axis_index("row"), lax.axis_index("col")
    me = r * plan.nc + c
    count = plan.count
    barrier = pltpu.get_barrier_semaphore()

    def device(d):
        other = lax.rem(me + d, count)
        return (other // plan.nc, lax.rem(other, plan.nc))

    def fetch(k):
        return pltpu.make_async_copy(b_hbm.at[k], braw.at[pl.ds(pl.multiple_of(k * plan.pitch, 8), rows)], in_sem.at[k])

    def fetch_start(k, carry):
        fetch(k).start()
        return carry

    def fetch_wait(k, carry):
        fetch(k).wait()
        return carry

    lax.fori_loop(0, n, fetch_start, 0)
    for ref in (ga, gb, gc, brow, bcol, ccol, gset0, gset1, gset2, gside0, gside1, gside2):
        ref[...] = jnp.zeros_like(ref)
    u1[0:n, :] = jnp.zeros((n, cols), F32)
    u1[(rows + 1) * n :, :] = jnp.zeros((n, cols), F32)

    def greet(d, carry):
        pl.semaphore_signal(barrier, inc=1, device_id=device(d), device_id_type=pl.DeviceIdType.MESH)
        return carry

    lax.fori_loop(1, count, greet, 0)

    i, j = iota((rows, cols), 0), iota((rows, cols), 1)
    row_end = jnp.where(r == plan.nr - 1, rows - 1, rows)
    col_end = jnp.where(c == plan.nc - 1, cols - 1, cols)
    planes[CO + 1] = jnp.where(j == col_end, 0.0, looked_up(edge_table, h_ref[...]))
    planes[CO + 3] = jnp.where(i == row_end, 0.0, looked_up(edge_table, v_ref[...]))
    for ref in (ea, eb, ec):
        ref[...] = jnp.zeros_like(ref)
    put_edges(ea, 0, label_ref[...].astype(F32))
    put_edges(ea, 1, bump_ref[...])
    put_edges(ea, 2, planes[CO + 1])
    put_edges(ea, 3, planes[CO + 3])
    legs = Legs(plan, send_sem, recv_sem)
    first_edges = legs.make(beside(ea, ga))
    base_row, base_col = windows(plan)
    bump = bump_ref[...]
    for k, hit in enumerate(hits_of(label_ref[...].astype(F32), base_row, base_col)):
        planes[Z + k] = jnp.where(hit, bump, 0.0)
    pl.semaphore_wait(barrier, count - 1)
    legs.start(first_edges)

    for ref in (s0, s1, s2, s3, s4, pa, pb, pc):
        ref[...] = jnp.zeros_like(ref)
    lax.fori_loop(0, n, fetch_wait, 0)

    lane = iota((hn, cols), 1)
    even = lane % 2 == 0
    zero = jnp.zeros((hn, cols), F32)

    def own(h):
        return slice(h * hn, (h + 1) * hn)

    def spot(h, k):
        return pl.ds(pl.multiple_of(k * n + h * hn, 8), hn)

    def keep_ends(ref, h, field, skip):
        pack, top = [zero, zero], None
        for k in range(rows):
            moved = rolled(field[spot(h, k + skip), :], k, 1)
            top = moved if k == 0 else top
            pack[k % 2] = moved if k < 2 else jnp.where(lane >= k - 1, moved, pack[k % 2])
        pack[0] = jnp.where(lane == cols - 1, top, pack[0])
        ref[0, own(h), :] = jnp.where(even, pack[1], pack[0])
        ref[1, own(h), :] = jnp.where(even, pack[0], pack[1])

    def halo_rows(h, from_left, from_right):
        from_left = -ga[2, 2:3, :] * from_left
        from_right = pltpu.roll(-ea[2, 2:3, :] * from_right, cols - 1, 1)
        pair = [jnp.where(even, from_left, from_right), jnp.where(even, from_right, from_left)]
        outer = (lane == 0) | (lane == cols - 1)
        for k in range(rows):
            beyond[spot(h, k), :] = jnp.where(outer, rolled(pair[k % 2], -k, 1), 0.0)

    for h in (0, 1):
        for part, first, last in plan.chunks():

            def group(base, acc):
                for u in range(8):
                    k = base + u
                    v = braw[pl.ds(k + h * hn * plan.pitch, hn, stride=plan.pitch), :]
                    bt[spot(h, k), :] = v
                    acc = tuple(x + row_of(planes, Z + m, k) * v for m, x in enumerate(acc))
                return acc

            add_sums(plan, s0, h, part, over_groups(first, last, group, (zero,) * 4))
        keep_ends(cpack, h, bt, 0)
    load_edges = legs.make([
        (1, 0, bt.at[pl.ds((rows - 1) * n, n)], brow.at[0]),
        (-1, 0, bt.at[pl.ds(0, n)], brow.at[1]),
        (0, 1, cpack.at[0], bcol.at[0]),
        (0, -1, cpack.at[1], bcol.at[1]),
    ])
    legs.start(load_edges)

    legs.wait(first_edges)
    around = Around(ga, rows, cols)
    right, down = planes[CO + 1], planes[CO + 3]
    left, upper = around.left(right, 2), around.top(down, 3)
    diagonal = looked_up(pad_table, pad_class_ref[...]) + right + left + down + upper
    minv = 1.0 / diagonal
    planes[CO] = diagonal
    planes[CO + 2] = left
    planes[RIGHT_IN] = jnp.where(j == cols - 1, 0.0, right)
    planes[LEFT_IN] = jnp.where(j == 0, 0.0, left)
    planes[CO + 4] = upper
    planes[MINV] = minv
    named = label_ref[...].astype(F32)
    bump = bump_ref[...]
    total = None
    for label, weight in (
        (named, diagonal * bump),
        (around.right(named, 0), -right * around.right(bump, 1)),
        (around.left(named, 0), -left * around.left(bump, 1)),
        (around.low(named, 0), -down * around.low(bump, 1)),
        (around.top(named, 0), -upper * around.top(bump, 1)),
    ):
        terms = [jnp.where(hit, weight, 0.0) for hit in hits_of(label, base_row, base_col)]
        total = terms if total is None else [t + u for t, u in zip(total, terms)]
    put_edges(eb, 0, minv)
    for k in range(4):
        planes[W0 + k] = total[k]
        value = total[k] * minv
        planes[V0 + k] = value
        put_edges(eb, 1 + k, value)
    image_edges = legs.make(beside(eb, gb))
    legs.start(image_edges)

    pair_sums(plan, planes, Z, W0, pa, 0)
    spread0 = Spread(plan, legs, set0, side0, gset0, gside0)
    spread0.send([packed(plan, s0), packed(plan, pa)])

    for h in (0, 1):
        dots = zero
        for part, first, last in plan.chunks():

            def step(k, u, carry):
                dots, acc = carry
                v = bt[spot(h, k), :]
                w = row_of(planes, MINV, k) * v
                u0[spot(h, k + 1), :] = w
                return dots + v * w, tuple(x + row_of(planes, V0 + m, k) * v for m, x in enumerate(acc))

            dots, acc = over_rows(first, last, step, (dots, (zero,) * 4))
            add_sums(plan, s1, h, part, acc)
        tacc[h * hn : (h + 1) * hn, :] = dots

    def note_copy(m, d):
        return pltpu.make_async_remote_copy(
            src_ref=note.at[m],
            dst_ref=gat.at[m, me],
            send_sem=note_send.at[m, d],
            recv_sem=note_recv.at[m, d],
            device_id=device(d),
            device_id_type=pl.DeviceIdType.MESH,
        )

    def tell(m, value):
        note[m] = value
        gat[m, pl.ds(me, 1)] = value[None]

        def go(d, carry):
            note_copy(m, d).start()
            return carry

        lax.fori_loop(1, count, go, 0)

    def hear(m):
        def go(d, carry):
            note_copy(m, d).wait()
            return carry

        lax.fori_loop(1, count, go, 0)

    legs.wait(load_edges)
    legs.wait(image_edges)
    u0[0:n, :] = brow[0] * gb[0, 0:1, :]
    u0[(rows + 1) * n :, :] = brow[1] * gb[1, 0:1, :]
    for h in (0, 1):
        halo_rows(h, pltpu.roll(bcol[0, own(h), :], 1, 1) * gb[2, 0:1, :], bcol[1, own(h), :] * gb[3, 0:1, :])
    around = Around(gb, rows, cols)
    for k, value in enumerate(around.images(plan, planes, V0, 1)):
        planes[W1 + k] = value
        value = value * planes[MINV]
        planes[V1 + k] = value
        put_edges(ec, k, value)
    next_edges = legs.make(beside(ec, gc))
    legs.start(next_edges)

    def stencil(field, h, k):
        z = field[spot(h, k + 1), :]
        f = (
            row_of(planes, CO, k) * z
            - row_of(planes, RIGHT_IN, k) * pltpu.roll(z, cols - 1, 1)
            - row_of(planes, LEFT_IN, k) * pltpu.roll(z, 1, 1)
            - row_of(planes, CO + 3, k) * field[spot(h, k + 2), :]
            - row_of(planes, CO + 4, k) * field[spot(h, k), :]
        )
        return z, f + beyond[spot(h, k), :]

    field_edges = []
    for h in (0, 1):
        dots, more = zero, zero
        for part, first, last in plan.chunks():

            def group(base, carry):
                dots, more, acc, bcc = carry
                for u in range(GROUP):
                    k = base + u
                    z, f = stencil(u0, h, k)
                    w = row_of(planes, MINV, k) * f
                    b1[spot(h, k), :] = f
                    u1[spot(h, k + 1), :] = w
                    acc = tuple(x + row_of(planes, V0 + m, k) * f for m, x in enumerate(acc))
                    bcc = tuple(x + row_of(planes, V1 + m, k) * f for m, x in enumerate(bcc))
                    dots, more = dots + z * f, more + w * f
                return dots, more, acc, bcc

            dots, more, acc, bcc = over_groups(first, last, group, (dots, more, (zero,) * 4, (zero,) * 4), GROUP)
            add_sums(plan, s2, h, part, acc)
            add_sums(plan, s3, h, part, bcc)
        tacc[n + h * hn : n + (h + 1) * hn, :] = dots
        tacc[2 * n + h * hn : 2 * n + (h + 1) * hn, :] = more
        keep_ends(cpack1, h, u1, 1)
        mine = pl.ds(h * hn, hn)
        field_edges.append(legs.make([
            (1, 0, u1.at[pl.ds(rows * n + h * hn, hn)], u1.at[pl.ds(h * hn, hn)]),
            (-1, 0, u1.at[pl.ds(n + h * hn, hn)], u1.at[pl.ds((rows + 1) * n + h * hn, hn)]),
            (0, 1, cpack1.at[0, mine], ccol.at[0, mine]),
            (0, -1, cpack1.at[1, mine], ccol.at[1, mine]),
        ]))
        legs.start(field_edges[h])
        if h == 0:
            load_sums, energy = spread0.merged()
            tell(0, message(plan, [(0, load_sums), (1, energy)]))
    out1 = pltpu.make_async_copy(b1, b1_out, out_sem.at[0])
    out1.start()

    pair_sums(plan, planes, W0, V0, pb, 0)
    pair_sums(plan, planes, W1, V0, pb, 9)
    pair_sums(plan, planes, W1, V1, pb, 18)
    spread1 = Spread(plan, legs, set1, side1, gset1, gside1)
    spread1.send([packed(plan, s1), packed(plan, s2), packed(plan, s3), packed(plan, pb)])

    legs.wait(next_edges)
    around = Around(gc, rows, cols)
    for k, value in enumerate(around.images(plan, planes, V1, 0)):
        planes[W2 + k] = value
    out0 = pltpu.make_async_copy(planes.at[pl.ds(0, KEPT)], planes_out, out_sem.at[1])
    out0.start()
    for h in (0, 1):
        legs.wait(field_edges[h])
        halo_rows(h, pltpu.roll(ccol[0, own(h), :], 1, 1), ccol[1, own(h), :])
        dots = zero
        for part, first, last in plan.chunks():

            def group(base, carry):
                dots, acc = carry
                for u in range(GROUP):
                    k = base + u
                    z, f = stencil(u1, h, k)
                    b2[spot(h, k), :] = f
                    dots = dots + z * f
                    acc = tuple(x + row_of(planes, V1 + m, k) * f for m, x in enumerate(acc))
                return dots, acc

            dots, acc = over_groups(first, last, group, (dots, (zero,) * 4), GROUP)
            add_sums(plan, s4, h, part, acc)
        tacc[3 * n + h * hn : 3 * n + (h + 1) * hn, :] = dots
    out2 = pltpu.make_async_copy(b2, b2_out, out_sem.at[2])
    out2.start()
    pair_sums(plan, planes, W2, V1, pc, 0)
    spread2 = Spread(plan, legs, set2, side2, gset2, gside2)
    spread2.send([packed(plan, pc), packed(plan, s4)])
    dots = jnp.sum(tacc[...].T, axis=0, keepdims=True)

    first_sums, second_sums, third_sums, pairs = spread1.merged()
    tell(1, message(plan, [(0, first_sums), (1, second_sums), (2, third_sums), (3, pairs)]))

    def settle(m, ref):
        hear(m)
        for d in range(count):
            for l in range(plan.lv):
                at = REG * ORDER.index(d // plan.nc * plan.lv + l) + d % plan.nc * plan.cw
                ref[at : at + plan.cw, :] = gat[m, d, l * plan.cw : (l + 1) * plan.cw, :]

    def last_message():
        last_pairs, last_sums = spread2.merged()
        value = message(plan, [(0, last_pairs), (3, last_sums)])
        sub, block = iota((8, LANES), 0), iota((8, LANES), 1) // BLOCK
        for k in range(4):
            value = jnp.where((sub == k) & (block == 1), rolled(dots, BLOCK * (1 - k), 1), value)
        tell(2, value)

    settle(0, q0)
    inverse = whole_inverse(coarse_matrix(q0[...], BLOCK), last_message)
    c0 = same(dot(inverse, q0[...]), 0)
    settle(1, q1)
    settle(2, q2)

    regions = c0.shape[0]
    block = iota((regions, LANES), 1) // BLOCK
    pair_values = jnp.where(block == 3, q1[...], q2[...])
    sums = jnp.where(block == 3, q2[...], q1[...])
    start = jnp.where(block == 3, 0, 3 * BLOCK + 9 * block)
    for k in range(9):
        diag[k] = taken(pair_values, start + k)
    all_dots = jnp.sum(gat[2], axis=0)
    row_block = iota((1, LANES), 1) // BLOCK
    dots = jnp.zeros((1, LANES), F32)
    for k in range(4):
        dots = jnp.where(row_block == k, rolled(all_dots[k : k + 1], BLOCK * (k - 1), 1), dots)

    def over(value):
        return jnp.sum(value, axis=0, keepdims=True)

    cpad[...] = jnp.zeros_like(cpad)
    cpad[8 : 8 + regions, :] = c0
    reduced = sums - banded(diag, cpad)
    dots = dots - over(c0 * (sums + reduced))
    rho, m1, m2, m3 = [same(dots, k) for k in range(4)]
    solved = dot(inverse, reduced)
    c1, e2 = same(solved, 0), same(solved, 1)
    cpad[8 : 8 + regions, :] = c1
    image = banded(diag, cpad)
    in_c1 = over(c1 * reduced)
    image_c1 = over(c1 * image)
    with_s1, with_s2, with_s3 = [same(in_c1, k) for k in range(3)]
    curve = m1 - with_s1
    alpha = rho / curve
    square = m2 - 2.0 * with_s2 + same(image_c1, 0)
    turned = same(dot(inverse, image), 0)
    c2 = c1 - alpha * (e2 - turned)
    now = reduced - alpha * (pltpu.roll(reduced, 3 * BLOCK, 1) - image)
    in_c2 = same(over(c2 * now), 0)
    image_dot = m1 - 2.0 * alpha * (m2 - with_s2) + alpha * alpha * (m3 - 2.0 * with_s3 + same(image_c1, 1))
    rho1 = rho - 2.0 * alpha * curve + alpha * alpha * square
    beta = rho1 / rho
    curve1 = image_dot - in_c2 + 2.0 * beta * (curve - alpha * square) + beta * beta * curve
    alpha1 = rho1 / curve1
    mix = alpha + alpha1 * beta
    kappa, lam = mix + alpha1, alpha * alpha1
    coefs = jnp.where(block == 0, c0 - mix * c1 - alpha1 * c2, jnp.where(block == 1, lam * c1 - kappa * c0, lam * c0))
    wide_ref[0] = wide(kappa)
    wide_ref[1] = wide(lam)

    knat[...] = jnp.zeros_like(knat)
    for q in range(REG):
        at = REG * (1 + ORDER[q])
        knat[at : at + REG, :] = coefs[q * REG : (q + 1) * REG]
    near = knat[pl.ds(pl.multiple_of(r * (plan.lv * REG), REG), LANES), :].T
    base = c * plan.cw - 1 + (iota((3 * BLOCK, cols), 1) + plan.width // 2) // plan.width
    for b in (0, 1):
        column = jnp.clip(base + b, 0, REG - 1)
        for l in range(plan.levels):
            value = taken(near[: 3 * BLOCK], column + l * REG)
            for f in range(3):
                cx_ref[f, b, l * n : (l + 1) * n, :] = value[f * BLOCK : f * BLOCK + n]

    out0.wait()
    out1.wait()
    out2.wait()
    legs.finish()


def last_kernel(
    plan, b_hbm, b1_hbm, b2_hbm, planes_hbm, cx_ref, wide_ref, x_hbm, r_hbm,
    braw, b1, b2, planes, xs, rs, in_sem, out_sem,
):
    n, hn = plan.loads, plan.half
    flat_b = braw.reshape(n * plan.pitch, plan.cols)
    flat_x = xs.reshape(n * plan.pitch, plan.cols)
    flat_r = rs.reshape(n * plan.pitch, plan.cols)
    arrivals, departures = [], []
    for part, first, last in plan.chunks():
        here, flat = pl.ds(first, last - first), pl.ds(first * n, (last - first) * n)
        arrivals.append([
            pltpu.make_async_copy(src, dst, in_sem.at[part, k])
            for k, (src, dst) in enumerate((
                (planes_hbm.at[:, here], planes.at[:, here]),
                (b_hbm.at[:, here], braw.at[:, here]),
                (b1_hbm.at[flat], b1.at[flat]),
                (b2_hbm.at[flat], b2.at[flat]),
            ))
        ])
        departures.append([
            pltpu.make_async_copy(xs.at[:, here], x_hbm.at[:, here], out_sem.at[part, 0]),
            pltpu.make_async_copy(rs.at[:, here], r_hbm.at[:, here], out_sem.at[part, 1]),
        ])
    for copies in arrivals:
        for copy in copies:
            copy.start()
    for part, first, last in plan.chunks():
        for copy in arrivals[part]:
            copy.wait()
        for h in (0, 1):
            kappa, lam = [wide_ref[k, h * hn : (h + 1) * hn, :] for k in (0, 1)]
            cx = []
            for f in range(3):
                for a in (0, 1):
                    for b in (0, 1):
                        at = (part + a) * n + h * hn
                        cx.append(cx_ref[f, b, at : at + hn, :])

            def step(k, u, carry):
                at = pl.ds(pl.multiple_of(k * n + h * hn, 8), hn)
                to = pl.ds(k + h * hn * plan.pitch, hn, stride=plan.pitch)
                v0, v1, v2 = flat_b[to, :], b1[at, :], b2[at, :]
                x = kappa * v0 - lam * v1
                r = v0 - kappa * v1 + lam * v2
                plain = None
                for m in range(4):
                    w0 = row_of(planes, W0 + m, k)
                    w1 = row_of(planes, W1 + m, k)
                    x = x + w0 * cx[4 + m] + w1 * cx[8 + m]
                    r = r - w0 * cx[m] - w1 * cx[4 + m] - row_of(planes, W2 + m, k) * cx[8 + m]
                    term = row_of(planes, Z + m, k) * cx[m]
                    plain = term if plain is None else plain + term
                flat_x[to, :] = row_of(planes, MINV, k) * x + plain
                flat_r[to, :] = r
                return carry

            over_rows(first, last, step, 0, 4)
        for copy in departures[part]:
            copy.start()
    for copies in departures:
        for copy in copies:
            copy.wait()


def body(load_currents, labels, bump_height, horizontal_class, vertical_class, pad_class, edge_table, pad_table):
    rows, cols = labels.shape
    loads = load_currents.shape[0]
    nr, nc = lax.axis_size("row"), lax.axis_size("col")
    height, width = nr * rows // REG, nc * cols // REG
    plan = Plan(rows, cols, loads, height, width, nr, nc)
    n, regions, count = loads, REG * REG, plan.count
    field = (rows * n, cols)
    tall = ((rows + 2) * n, cols)
    edge = (4, 8, cols)
    sums = (2, LANES, cols)

    def vm(*dims):
        return pltpu.VMEM(dims, F32)

    def dma(*dims):
        return pltpu.SemaphoreType.DMA(dims)

    legs = 4 * 6 + 3 * 8
    b1, b2, planes, cx, scales = pl.pallas_call(
        functools.partial(front_kernel, plan),
        out_shape=(shape(*field), shape(*field), shape(KEPT, rows, cols), shape(3, 2, plan.levels * n, cols), shape(2, n, cols)),
        in_specs=[ANY] + [VM] * 5 + [SM] * 2,
        out_specs=(ANY, ANY, ANY, VM, VM),
        scratch_shapes=[
            vm(n * plan.pitch, cols), vm(*field), vm(*tall), vm(*tall), vm(*field), vm(*field), vm(PLANES, rows, cols),
            vm(*edge), vm(*edge), vm(*edge), vm(*edge), vm(*edge), vm(*edge),
            vm(2, n, cols), vm(2, n, cols), vm(2, n, cols), vm(2, n, cols), vm(2, n, cols), vm(*field),
        ] + [vm(*sums)] * 8 + [
            vm(LANES, LANES),
            vm(2, 8, LANES), vm(4, 8, LANES), vm(2, 8, LANES), vm(2, 8, LANES), vm(2, 8, LANES), vm(2, 8, LANES),
            vm(2, 2, 8, LANES), vm(2, 4, 8, LANES), vm(2, 2, 8, LANES), vm(6, 8, LANES), vm(6, 8, LANES), vm(6, 8, LANES),
            vm(3, 8, LANES), vm(3, count, 8, LANES), vm(regions, LANES), vm(regions, LANES), vm(regions, LANES),
            vm(regions + 16, LANES), vm(9, regions, LANES), vm(regions + LANES + 2 * REG, LANES),
            dma(n), dma(3), dma(legs), dma(legs), dma(3, count), dma(3, count),
        ],
        compiler_params=pltpu.CompilerParams(collective_id=0, has_side_effects=True, vmem_limit_bytes=56 * 1024 * 1024),
    )(load_currents, horizontal_class, vertical_class, labels, bump_height, pad_class, edge_table, pad_table)
    staged = (n, plan.pitch, cols)
    return pl.pallas_call(
        functools.partial(last_kernel, plan),
        out_shape=(shape(n, rows, cols),) * 2,
        in_specs=[ANY] * 4 + [VM] * 2,
        out_specs=(ANY, ANY),
        scratch_shapes=[
            vm(*staged), vm(*field), vm(*field), vm(KEPT, rows, cols), vm(*staged), vm(*staged),
            dma(plan.parts, 4), dma(plan.parts, 2),
        ],
        compiler_params=pltpu.CompilerParams(vmem_limit_bytes=56 * 1024 * 1024),
    )(load_currents, b1, b2, planes, cx, scales)


def solution(mesh):
    grid = P("row", "col")
    cube = P(None, "row", "col")
    return jax.shard_map(
        body,
        mesh=mesh,
        in_specs=(cube, grid, grid, grid, grid, grid, P(), P()),
        out_specs=(cube, cube),
        check_vma=False,
    )
```

```python
import functools

import jax
import jax.numpy as jnp
from jax import lax
from jax.experimental import pallas as pl
from jax.experimental.pallas import tpu as pltpu
from jax.sharding import PartitionSpec as P

REG = 16
F32 = jnp.float32
HBM = pl.BlockSpec(memory_space=pltpu.HBM)
BLOCK = 32
LANES = 4 * BLOCK
PITCH = 8
GROUP = 32
MINV, Z, W0, W1, W2, V0, V1, CO = 0, 1, 5, 9, 13, 17, 21, 25
KEPT, PLANES = 17, 32
RIGHT_IN, LEFT_IN = 30, 31
ORDER = (0, 2, 4, 6, 8, 10, 12, 14, 1, 5, 9, 13, 3, 11, 7, 15)


def shape(*dims):
    return jax.ShapeDtypeStruct(dims, F32)


def iota(dims, axis):
    return lax.broadcasted_iota(jnp.int32, dims, axis)


def rolled(value, shift, axis):
    shift = shift % value.shape[axis]
    return pltpu.roll(value, shift, axis) if shift else value


class Plan:
    def __init__(self, rows, cols, loads, height, width, row_devices, col_devices):
        self.rows, self.cols, self.loads = rows, cols, loads
        self.height, self.width = height, width
        self.nr, self.nc = row_devices, col_devices
        self.count = row_devices * col_devices
        self.lv, self.cw = rows // height, cols // width
        self.parts = self.lv + 1
        self.levels = self.lv + 2
        self.half = loads // 2
        self.pitch = rows + PITCH

    def chunks(self):
        half = self.height // 2
        for part in range(self.parts):
            yield part, max(0, part * self.height - half), min(self.rows, part * self.height + half)

    def pieces(self):
        for part, first, last in self.chunks():
            cut = first + 8 if part == 0 else last - 8 if part == self.parts - 1 else first
            for start, stop in ((first, cut), (cut, last)):
                if stop > start:
                    yield part, start, stop


def over_rows(first, last, step, init, group=4):
    def body(g, carry):
        for u in range(group):
            carry = step(first + g * group + u, u, carry)
        return carry

    return lax.fori_loop(0, (last - first) // group, body, init)


def over_groups(first, last, group, init, size=8):
    return lax.fori_loop(0, (last - first) // size, lambda g, carry: group(first + g * size, carry), init)


def row_of(ref, k, i):
    return ref[k, pl.ds(i, 1), :]


class Legs:
    def __init__(self, plan, send_sem, recv_sem):
        self.plan, self.send_sem, self.recv_sem = plan, send_sem, recv_sem
        self.used = 0
        self.r, self.c = lax.axis_index("row"), lax.axis_index("col")

    def inside(self, dr, dc):
        r, c = self.r + dr, self.c + dc
        return (r >= 0) & (r < self.plan.nr) & (c >= 0) & (c < self.plan.nc)

    def make(self, items, sends):
        out = []
        for dr, dc, src, dst in items:
            target = (lax.rem(self.r + dr + self.plan.nr, self.plan.nr), lax.rem(self.c + dc + self.plan.nc, self.plan.nc))
            copy = pltpu.make_async_remote_copy(
                src_ref=src,
                dst_ref=dst,
                send_sem=self.send_sem.at[sends + len(out)],
                recv_sem=self.recv_sem.at[self.used],
                device_id=target,
                device_id_type=pl.DeviceIdType.MESH,
            )
            self.used += 1
            out.append((self.inside(dr, dc), self.inside(-dr, -dc), copy))
        return out

    def start(self, legs):
        for goes, _, copy in legs:
            pl.when(goes)(copy.start)

    def wait(self, legs):
        for _, comes, copy in legs:
            pl.when(comes)(copy.wait_recv)

    def sent(self, legs):
        for goes, _, copy in legs:
            pl.when(goes)(copy.wait_send)


def beside(src, dst):
    return [(1, 0, src.at[0], dst.at[0]), (-1, 0, src.at[1], dst.at[1]), (0, 1, src.at[2], dst.at[2]), (0, -1, src.at[3], dst.at[3])]


def looked_up(table_ref, classes):
    out = jnp.zeros(classes.shape, F32)
    for k in range(table_ref.shape[0]):
        out = jnp.where(classes == k, table_ref[k], out)
    return out


def put_edges(ref, k, value, row_end=True):
    rows, cols = value.shape
    ref[0, k : k + 1, :] = value[rows - 1 :]
    ref[1, k : k + 1, :] = value[:1]
    turned = value.T
    ref[2, k : k + 1, :] = turned[cols - 1 :]
    ref[3, k : k + 1, :] = turned[:1]


class Around:
    def __init__(self, edge_ref, rows, cols):
        self.edge_ref, self.rows, self.cols = edge_ref, rows, cols
        self.i, self.j = iota((rows, cols), 0), iota((rows, cols), 1)

    def column(self, side, k):
        return jnp.broadcast_to(self.edge_ref[side, k : k + 1, :], (self.cols, self.rows)).T

    def left(self, value, k):
        return jnp.where(self.j == 0, self.column(2, k), pltpu.roll(value, 1, 1))

    def right(self, value, k):
        return jnp.where(self.j == self.cols - 1, self.column(3, k), pltpu.roll(value, self.cols - 1, 1))

    def top(self, value, k):
        return jnp.where(self.i == 0, self.edge_ref[0, k : k + 1, :], pltpu.roll(value, 1, 0))

    def low(self, value, k):
        return jnp.where(self.i == self.rows - 1, self.edge_ref[1, k : k + 1, :], pltpu.roll(value, self.rows - 1, 0))

    def turns(self, at, size, step):
        out = None
        for p in range(1, size // step + 1):
            hit = at == p * step - step // 2
            out = hit if out is None else out | hit
        return out

    def images(self, plan, planes, source, k):
        values = [planes[source + m] for m in range(4)]
        to_right = self.turns(self.j + 1, plan.cols, plan.width)
        to_left = self.turns(self.j, plan.cols, plan.width)
        to_low = self.turns(self.i + 1, plan.rows, plan.height)
        to_top = self.turns(self.i, plan.rows, plan.height)

        def shifted(reader, turn, step, later):
            seen = [reader(value, k + m) for m, value in enumerate(values)]
            out = list(seen)
            for m in range(4):
                if bool(m & step) == later:
                    out[m] = jnp.where(turn, seen[m ^ step], seen[m])
                else:
                    out[m] = jnp.where(turn, 0.0, seen[m])
            return out

        right = shifted(self.right, to_right, 1, True)
        left = shifted(self.left, to_left, 1, False)
        low = shifted(self.low, to_low, 2, True)
        top = shifted(self.top, to_top, 2, False)
        return [
            planes[CO] * values[m]
            - planes[CO + 1] * right[m]
            - planes[CO + 2] * left[m]
            - planes[CO + 3] * low[m]
            - planes[CO + 4] * top[m]
            for m in range(4)
        ]


def windows(plan):
    rows, cols = plan.rows, plan.cols
    i, j = iota((rows, cols), 0), iota((rows, cols), 1)
    base_row = jnp.zeros((rows, cols), F32) + (lax.axis_index("row") * plan.lv - 1).astype(F32)
    base_col = jnp.zeros((rows, cols), F32) + (lax.axis_index("col") * plan.cw - 1).astype(F32)
    for p in range(1, plan.parts):
        base_row = base_row + jnp.where(i >= p * plan.height - plan.height // 2, 1.0, 0.0)
    for p in range(1, plan.cw + 1):
        base_col = base_col + jnp.where(j >= p * plan.width - plan.width // 2, 1.0, 0.0)
    return base_row, base_col


def hits_of(label, base_row, base_col):
    high = jnp.floor(label * (1.0 / REG))
    a, b = high - base_row, label - REG * high - base_col
    return [(a == m) & (b == n) for m in (0.0, 1.0) for n in (0.0, 1.0)]


def add_sums(plan, s_ref, h, part, acc):
    n, hn = plan.loads, plan.half
    for a in (0, 1):
        for b in (0, 1):
            at = (part + a) * n + h * hn
            s_ref[b, at : at + hn, :] = s_ref[b, at : at + hn, :] + acc[2 * a + b]


def packed(plan, s_ref):
    out = [None] * (plan.cw + 2)
    half = plan.width // 2
    for b in (0, 1):
        turned = s_ref[b].T
        for g in range(plan.cw + 1):
            part = turned[max(0, g * plan.width - half) : min(plan.cols, g * plan.width + half)]
            term = jnp.sum(part, axis=0, keepdims=True)
            out[g + b] = term if out[g + b] is None else out[g + b] + term
    out.append(jnp.zeros((8 - len(out), LANES), F32))
    return jnp.concatenate(out, axis=0)


def pair_sums(plan, planes, x, y, pair_ref, q):
    terms = {}
    for part, first, last in plan.chunks():
        for k in range(4):
            for m in range(4):
                da, db = m // 2 - k // 2, m % 2 - k % 2
                at = (k % 2, (part + k // 2) * BLOCK + q + (da + 1) * 3 + db + 1)
                term = jnp.sum(planes[x + k, first:last, :] * planes[y + m, first:last, :], axis=0, keepdims=True)
                terms[at] = term if at not in terms else terms[at] + term
    for (b, at), term in terms.items():
        pair_ref[b, at : at + 1, :] = term


class Spread:
    def __init__(self, plan, legs, planes, sides, got_planes, got_sides):
        self.plan, self.planes, self.sides = plan, planes, sides
        self.got_planes, self.got_sides = got_planes, got_sides
        west, east = sides.at[0], sides.at[1]
        self.legs = legs
        self.mine = legs.make([
            (1, 0, planes, got_planes.at[0]),
            (-1, 0, planes, got_planes.at[1]),
            (0, -1, west, got_sides.at[0]),
            (1, -1, west, got_sides.at[1]),
            (-1, -1, west, got_sides.at[2]),
            (0, 1, east, got_sides.at[3]),
            (1, 1, east, got_sides.at[4]),
            (-1, 1, east, got_sides.at[5]),
        ], 12)

    def send(self, values):
        last = self.plan.cw + 1
        for k, value in enumerate(values):
            self.planes[k] = value
            self.sides[0, k : k + 1, :] = value[:1]
            self.sides[1, k : k + 1, :] = value[last : last + 1]
        self.legs.start(self.mine)

    def meet(self, own, above, below):
        lv = self.plan.lv
        block = iota(own.shape, len(own.shape) - 1) // BLOCK
        shift = lv * BLOCK
        return own + jnp.where(block == 1, rolled(above, -shift, 1), 0.0) + jnp.where(block == lv, rolled(below, shift, 1), 0.0)

    def merged(self, early=False):
        self.legs.wait(self.mine)
        if not early:
            self.legs.sent(self.mine)
        sub = iota((8, LANES), 0)
        sides = self.got_sides
        right = self.meet(sides[0], sides[1], sides[2])
        left = self.meet(sides[3], sides[4], sides[5])
        out = []
        for k in range(self.planes.shape[0]):
            value = self.meet(self.planes[k], self.got_planes[0, k], self.got_planes[1, k])
            value = value + jnp.where(sub == self.plan.cw, right[k : k + 1], 0.0) + jnp.where(sub == 1, left[k : k + 1], 0.0)
            out.append(value)
        return out


def message(plan, pieces):
    sub, block = iota((8, LANES), 0), iota((8, LANES), 1) // BLOCK
    out = jnp.zeros((8, LANES), F32)
    for spot, value in pieces:
        for l in range(plan.lv):
            first = l * plan.cw
            moved = rolled(rolled(value, first - 1, 0), BLOCK * (spot - 1 - l), 1)
            out = jnp.where((block == spot) & (sub >= first) & (sub < first + plan.cw), moved, out)
    return out


def fold(value):
    half = value + pltpu.roll(value, 2 * BLOCK, 1)
    return half + pltpu.roll(half, BLOCK, 1)


def same(value, spot):
    return fold(jnp.where(iota(value.shape, 1) // BLOCK == spot, value, 0.0))


def halves(value):
    high = value.astype(jnp.bfloat16)
    return high, (value - high.astype(F32)).astype(jnp.bfloat16)


def dot(a, b, contract=((1,), (0,))):
    (a_high, a_low), (b_high, b_low) = halves(a), halves(b)
    total = None
    for left, right in ((a_high, b_low), (a_low, b_high), (a_high, b_high)):
        term = lax.dot_general(left, right, (contract, ((), ())), preferred_element_type=F32)
        total = term if total is None else total + term
    return total


def taken(value, index):
    return jnp.take_along_axis(value, index, axis=1, mode="promise_in_bounds")


def small_inverses(value):
    lane, sub = iota(value.shape, 1), iota(value.shape, 0)
    start = lane // REG * REG
    cols = [taken(value, start + j) for j in range(REG)]
    for k in range(REG):
        col = cols[k]
        here = sub == k
        recip = 1.0 / col[k : k + 1]
        left = jnp.where(here, -1.0, col)
        for j in range(REG):
            if j != k:
                row = cols[j][k : k + 1] * recip
                cols[j] = jnp.where(here, 0.0, cols[j]) - left * row
        cols[k] = jnp.where(here, recip, -col * recip)
    out = cols[0]
    for j in range(1, REG):
        out = jnp.where(lane % REG == j, cols[j], out)
    return out


def block_inverses(matrix, first, count):
    width = matrix.shape[1]
    lane, sub = iota((REG, width), 1), iota((REG, width), 0)
    value = jnp.where(lane % REG == sub, 1.0, 0.0)
    for q in range(first, first + count):
        value = jnp.where(lane // REG == q, matrix[q * REG : (q + 1) * REG], value)
    value = small_inverses(value)
    return jnp.concatenate([jnp.where(lane // REG == q, value, 0.0) for q in range(first, first + count)], axis=0)


def placed(value, first, total):
    pieces = []
    if first:
        pieces.append(jnp.zeros((first, value.shape[1]), F32))
    pieces.append(value)
    rest = total - first - value.shape[0]
    if rest:
        pieces.append(jnp.zeros((rest, value.shape[1]), F32))
    return jnp.concatenate(pieces, axis=0) if len(pieces) > 1 else value


def tail_inverse(matrix, first, count, between):
    size = matrix.shape[0]
    if count == 1:
        return block_inverses(matrix, first, 1)
    a, b, c = first * REG, (first + count // 2) * REG, (first + count) * REG
    lane = iota((1, size), 1)
    early, late = (lane >= a) & (lane < b), (lane >= b) & (lane < c)
    x = block_inverses(matrix, first, count // 2)
    f = placed(jnp.where(late, matrix[a:b], 0.0), a, size)
    y = dot(x, f)
    y_full = placed(y, a, size)
    rest = matrix[b:c] - dot(jnp.where(early, matrix[b:c], 0.0), y_full)
    rest = jnp.where(late, rest, 0.0)
    if count == 2:
        between()
    inner = tail_inverse(placed(rest, b, size), first + count // 2, count // 2, between)
    t = dot(y, placed(inner, b, size))
    top = jnp.where(early, x + dot(t, y_full, ((1,), (1,))), -t)
    turned = placed(t, a, size).T
    low = jnp.where(early, -turned[b:c], inner)
    return jnp.concatenate([top, low], axis=0)


def whole_inverse(matrix, between):
    half = matrix.shape[0] // 2
    x = block_inverses(matrix[:half, :half], 0, half // REG)
    y = dot(x, matrix[:half, half:])
    rest = matrix[half:, half:] - dot(matrix[half:, :half], y)
    inner = tail_inverse(rest, 0, half // REG, between)
    t = dot(y, inner)
    top = jnp.concatenate([x + dot(t, y, ((1,), (1,))), -t], axis=1)
    return jnp.concatenate([top, jnp.concatenate([-t.T, inner], axis=1)], axis=0)


def region_of(at):
    q = at // REG
    row = jnp.where(q < 8, 2 * q, jnp.where(q < 12, 4 * q - 31, jnp.where(q < 14, 8 * q - 93, jnp.where(q < 15, 7, 15))))
    return row * REG + at % REG


def coarse_matrix(value, first):
    size = value.shape[0]
    gap = region_of(iota((size, size), 1)) - region_of(iota((size, size), 0))
    total = jnp.zeros((size, size), F32)
    for k in range(9):
        total = jnp.where(gap == REG * (k // 3 - 1) + k % 3 - 1, value[:, first + k : first + k + 1], total)
    return total


def banded(diag_ref, pad_ref):
    out = []
    for q in range(REG):
        total = None
        for k in range(9):
            row = ORDER[q] + k // 3 - 1
            if 0 <= row < REG:
                at = 8 + REG * ORDER.index(row) + k % 3 - 1
                term = diag_ref[k, q * REG : (q + 1) * REG, :] * pad_ref[at : at + REG, :]
                total = term if total is None else total + term
        out.append(total)
    return jnp.concatenate(out, axis=0)


def wide(value):
    return jnp.broadcast_to(value, (LANES, LANES)).T[:BLOCK]


def front_kernel(
    plan, b_hbm, h_hbm, v_hbm, label_hbm, bump_hbm, pad_class_hbm, edge_hbm, pad_hbm,
    b1_out, b2_out, planes_out, cx_out,
    h_ref, v_ref, label_ref, bump_ref, pad_class_ref, edge_table, pad_table, braw, bt, u0, u1, b1, b2, planes, ea, eb, ec, ga, gb, gc, brow, bcol, ccol, cpack, cpack1, beyond,
    s0, s1, s2, s3, s4, pa, pb, pc, tacc,
    set0, set1, set2, side0, side1, side2, gset0, gset1, gset2, gside0, gside1, gside2,
    note, gat, q0, q1, q2, cpad, cpad1, diag, knat, cx_ref,
    in_sem, small_sem, out_sem, send_sem, recv_sem, note_send, note_recv,
):
    rows, cols, n, hn = plan.rows, plan.cols, plan.loads, plan.half
    r, c = lax.axis_index("row"), lax.axis_index("col")
    me = r * plan.nc + c
    count = plan.count
    barrier = pltpu.get_barrier_semaphore()

    def device(d):
        other = lax.rem(me + d, count)
        return (other // plan.nc, lax.rem(other, plan.nc))

    def fetch(k):
        here, there = pl.ds(pl.multiple_of(k * rows, 8), rows), pl.ds(pl.multiple_of(k * plan.pitch, 8), rows)
        return pltpu.make_async_copy(b_hbm.at[here], braw.at[there], in_sem)

    def fetch_start(k, carry):
        fetch(k).start()
        return carry

    small = [
        pltpu.make_async_copy(src, dst, small_sem.at[k])
        for k, (src, dst) in enumerate((
            (h_hbm, h_ref), (edge_hbm, edge_table), (v_hbm, v_ref), (label_hbm, label_ref),
            (bump_hbm, bump_ref), (pad_class_hbm, pad_class_ref), (pad_hbm, pad_table),
        ))
    ]
    for copy in small:
        copy.start()
    lax.fori_loop(0, n, fetch_start, 0)
    for ref in (ga, gb, gc, brow, bcol, ccol, gset0, gset1, gset2, gside0, gside1, gside2):
        ref[...] = jnp.zeros_like(ref)
    u1[0:n, :] = jnp.zeros((n, cols), F32)
    u1[(rows + 1) * n :, :] = jnp.zeros((n, cols), F32)

    def greet(d, carry):
        pl.semaphore_signal(barrier, inc=1, device_id=device(d), device_id_type=pl.DeviceIdType.MESH)
        return carry

    lax.fori_loop(1, count, greet, 0)

    for copy in small:
        copy.wait()
    i, j = iota((rows, cols), 0), iota((rows, cols), 1)
    row_end = jnp.where(r == plan.nr - 1, rows - 1, rows)
    col_end = jnp.where(c == plan.nc - 1, cols - 1, cols)
    planes[CO + 1] = jnp.where(j == col_end, 0.0, looked_up(edge_table, h_ref[...]))
    planes[CO + 3] = jnp.where(i == row_end, 0.0, looked_up(edge_table, v_ref[...]))
    for ref in (ea, eb, ec):
        ref[...] = jnp.zeros_like(ref)
    put_edges(ea, 0, label_ref[...].astype(F32))
    put_edges(ea, 1, bump_ref[...])
    put_edges(ea, 2, planes[CO + 1])
    put_edges(ea, 3, planes[CO + 3])
    legs = Legs(plan, send_sem, recv_sem)
    first_edges = legs.make(beside(ea, ga), 0)
    base_row, base_col = windows(plan)
    bump = bump_ref[...]
    for k, hit in enumerate(hits_of(label_ref[...].astype(F32), base_row, base_col)):
        planes[Z + k] = jnp.where(hit, bump, 0.0)
    pl.semaphore_wait(barrier, count - 1)
    legs.start(first_edges)

    for ref in (s0, s1, s2, s3, s4, pa, pb, pc):
        ref[...] = jnp.zeros_like(ref)
    pltpu.make_async_copy(b_hbm, braw.at[pl.ds(0, n * rows)], in_sem).wait()

    lane = iota((hn, cols), 1)
    even = lane % 2 == 0
    zero = jnp.zeros((hn, cols), F32)

    def own(h):
        return slice(h * hn, (h + 1) * hn)

    def spot(h, k):
        return pl.ds(pl.multiple_of(k * n + h * hn, 8), hn)

    def keep_ends(ref, h, field, skip):
        pack, top = [zero, zero], None
        for k in range(rows):
            moved = rolled(field[spot(h, k + skip), :], k, 1)
            top = moved if k == 0 else top
            pack[k % 2] = moved if k < 2 else jnp.where(lane >= k - 1, moved, pack[k % 2])
        pack[0] = jnp.where(lane == cols - 1, top, pack[0])
        ref[0, own(h), :] = jnp.where(even, pack[1], pack[0])
        ref[1, own(h), :] = jnp.where(even, pack[0], pack[1])

    def halo_rows(h, from_left, from_right):
        from_left = -ga[2, 2:3, :] * from_left
        from_right = pltpu.roll(-ea[2, 2:3, :] * from_right, cols - 1, 1)
        pair = [jnp.where(even, from_left, from_right), jnp.where(even, from_right, from_left)]
        outer = (lane == 0) | (lane == cols - 1)
        for k in range(rows):
            beyond[spot(h, k), :] = jnp.where(outer, rolled(pair[k % 2], -k, 1), 0.0)

    for h in (0, 1):
        for part, first, last in plan.chunks():

            def group(base, acc):
                for u in range(8):
                    k = base + u
                    v = braw[pl.ds(k + h * hn * plan.pitch, hn, stride=plan.pitch), :]
                    bt[spot(h, k), :] = v
                    acc = tuple(x + row_of(planes, Z + m, k) * v for m, x in enumerate(acc))
                return acc

            add_sums(plan, s0, h, part, over_groups(first, last, group, (zero,) * 4))
        keep_ends(cpack, h, bt, 0)
    load_edges = legs.make([
        (1, 0, bt.at[pl.ds((rows - 1) * n, n)], brow.at[0]),
        (-1, 0, bt.at[pl.ds(0, n)], brow.at[1]),
        (0, 1, cpack.at[0], bcol.at[0]),
        (0, -1, cpack.at[1], bcol.at[1]),
    ], 4)
    legs.start(load_edges)

    legs.wait(first_edges)
    around = Around(ga, rows, cols)
    right, down = planes[CO + 1], planes[CO + 3]
    left, upper = around.left(right, 2), around.top(down, 3)
    diagonal = looked_up(pad_table, pad_class_ref[...]) + right + left + down + upper
    minv = 1.0 / diagonal
    planes[CO] = diagonal
    planes[CO + 2] = left
    planes[RIGHT_IN] = jnp.where(j == cols - 1, 0.0, right)
    planes[LEFT_IN] = jnp.where(j == 0, 0.0, left)
    planes[CO + 4] = upper
    planes[MINV] = minv
    named = label_ref[...].astype(F32)
    bump = bump_ref[...]
    total = None
    for label, weight in (
        (named, diagonal * bump),
        (around.right(named, 0), -right * around.right(bump, 1)),
        (around.left(named, 0), -left * around.left(bump, 1)),
        (around.low(named, 0), -down * around.low(bump, 1)),
        (around.top(named, 0), -upper * around.top(bump, 1)),
    ):
        terms = [jnp.where(hit, weight, 0.0) for hit in hits_of(label, base_row, base_col)]
        total = terms if total is None else [t + u for t, u in zip(total, terms)]
    put_edges(eb, 0, minv)
    for k in range(4):
        planes[W0 + k] = total[k]
        value = total[k] * minv
        planes[V0 + k] = value
        put_edges(eb, 1 + k, value)
    image_edges = legs.make(beside(eb, gb), 8)
    legs.start(image_edges)

    pair_sums(plan, planes, Z, W0, pa, 0)
    spread0 = Spread(plan, legs, set0, side0, gset0, gside0)
    spread0.send([packed(plan, s0), packed(plan, pa)])

    for h in (0, 1):
        dots = zero
        for part, first, last in plan.chunks():

            def step(k, u, carry):
                dots, acc = carry
                v = bt[spot(h, k), :]
                w = row_of(planes, MINV, k) * v
                u0[spot(h, k + 1), :] = w
                return dots + v * w, tuple(x + row_of(planes, V0 + m, k) * v for m, x in enumerate(acc))

            dots, acc = over_rows(first, last, step, (dots, (zero,) * 4))
            add_sums(plan, s1, h, part, acc)
        tacc[h * hn : (h + 1) * hn, :] = dots

    def note_copy(m, d):
        return pltpu.make_async_remote_copy(
            src_ref=note.at[m],
            dst_ref=gat.at[m, me],
            send_sem=note_send.at[m],
            recv_sem=note_recv.at[m],
            device_id=device(d),
            device_id_type=pl.DeviceIdType.MESH,
        )

    def tell(m, value):
        note[m] = value
        gat[m, pl.ds(me, 1)] = value[None]

        def go(d, carry):
            note_copy(m, d).start()
            return carry

        lax.fori_loop(1, count, go, 0)

    def hear(m):
        others = gat.at[m, pl.ds(0, count - 1)]
        every = pltpu.make_async_remote_copy(
            src_ref=others,
            dst_ref=others,
            send_sem=note_send.at[m],
            recv_sem=note_recv.at[m],
            device_id=device(1),
            device_id_type=pl.DeviceIdType.MESH,
        )
        every.wait_recv()
        every.wait_send()

    legs.wait(load_edges)
    legs.wait(image_edges)
    u0[0:n, :] = brow[0] * gb[0, 0:1, :]
    u0[(rows + 1) * n :, :] = brow[1] * gb[1, 0:1, :]
    for h in (0, 1):
        halo_rows(h, pltpu.roll(bcol[0, own(h), :], 1, 1) * gb[2, 0:1, :], bcol[1, own(h), :] * gb[3, 0:1, :])
    around = Around(gb, rows, cols)
    for k, value in enumerate(around.images(plan, planes, V0, 1)):
        planes[W1 + k] = value
        value = value * planes[MINV]
        planes[V1 + k] = value
        put_edges(ec, k, value)
    for gone in (first_edges, load_edges, image_edges):
        legs.sent(gone)
    next_edges = legs.make(beside(ec, gc), 0)
    legs.start(next_edges)

    def stencil(field, h, k):
        z = field[spot(h, k + 1), :]
        f = (
            row_of(planes, CO, k) * z
            - row_of(planes, RIGHT_IN, k) * pltpu.roll(z, cols - 1, 1)
            - row_of(planes, LEFT_IN, k) * pltpu.roll(z, 1, 1)
            - row_of(planes, CO + 3, k) * field[spot(h, k + 2), :]
            - row_of(planes, CO + 4, k) * field[spot(h, k), :]
        )
        return z, f + beyond[spot(h, k), :]

    field_edges = []
    for h in (0, 1):
        dots, more = zero, zero
        for part, first, last in plan.chunks():

            def group(base, carry):
                dots, more, acc, bcc = carry
                for u in range(GROUP):
                    k = base + u
                    z, f = stencil(u0, h, k)
                    w = row_of(planes, MINV, k) * f
                    b1[spot(h, k), :] = f
                    u1[spot(h, k + 1), :] = w
                    acc = tuple(x + row_of(planes, V0 + m, k) * f for m, x in enumerate(acc))
                    bcc = tuple(x + row_of(planes, V1 + m, k) * f for m, x in enumerate(bcc))
                    dots, more = dots + z * f, more + w * f
                return dots, more, acc, bcc

            dots, more, acc, bcc = over_groups(first, last, group, (dots, more, (zero,) * 4, (zero,) * 4), GROUP)
            add_sums(plan, s2, h, part, acc)
            add_sums(plan, s3, h, part, bcc)
        tacc[n + h * hn : n + (h + 1) * hn, :] = dots
        tacc[2 * n + h * hn : 2 * n + (h + 1) * hn, :] = more
        keep_ends(cpack1, h, u1, 1)
        mine = pl.ds(h * hn, hn)
        field_edges.append(legs.make([
            (1, 0, u1.at[pl.ds(rows * n + h * hn, hn)], u1.at[pl.ds(h * hn, hn)]),
            (-1, 0, u1.at[pl.ds(n + h * hn, hn)], u1.at[pl.ds((rows + 1) * n + h * hn, hn)]),
            (0, 1, cpack1.at[0, mine], ccol.at[0, mine]),
            (0, -1, cpack1.at[1, mine], ccol.at[1, mine]),
        ], 4 + 4 * h))
        legs.start(field_edges[h])
        if h == 0:
            load_sums, energy = spread0.merged()
            tell(0, message(plan, [(0, load_sums), (1, energy)]))
    out1 = pltpu.make_async_copy(b1, b1_out, out_sem.at[0])
    out1.start()

    pair_sums(plan, planes, W0, V0, pb, 0)
    pair_sums(plan, planes, W1, V0, pb, 9)
    pair_sums(plan, planes, W1, V1, pb, 18)
    spread1 = Spread(plan, legs, set1, side1, gset1, gside1)
    spread1.send([packed(plan, s1), packed(plan, s2), packed(plan, s3), packed(plan, pb)])

    legs.wait(next_edges)
    around = Around(gc, rows, cols)
    for k, value in enumerate(around.images(plan, planes, V1, 0)):
        planes[W2 + k] = value
    out0 = pltpu.make_async_copy(planes.at[pl.ds(0, KEPT)], planes_out, out_sem.at[1])
    out0.start()
    for h in (0, 1):
        legs.wait(field_edges[h])
        halo_rows(h, pltpu.roll(ccol[0, own(h), :], 1, 1), ccol[1, own(h), :])
        dots = zero
        for part, first, last in plan.chunks():

            def group(base, carry):
                dots, acc = carry
                for u in range(GROUP):
                    k = base + u
                    z, f = stencil(u1, h, k)
                    b2[spot(h, k), :] = f
                    dots = dots + z * f
                    acc = tuple(x + row_of(planes, V1 + m, k) * f for m, x in enumerate(acc))
                return dots, acc

            dots, acc = over_groups(first, last, group, (dots, (zero,) * 4), GROUP)
            add_sums(plan, s4, h, part, acc)
        tacc[3 * n + h * hn : 3 * n + (h + 1) * hn, :] = dots
    out2 = pltpu.make_async_copy(b2, b2_out, out_sem.at[2])
    out2.start()
    pair_sums(plan, planes, W2, V1, pc, 0)
    legs.sent(spread1.mine)
    spread2 = Spread(plan, legs, set2, side2, gset2, gside2)
    spread2.send([packed(plan, pc), packed(plan, s4)])
    dots = jnp.sum(tacc[...].T, axis=0, keepdims=True)

    first_sums, second_sums, third_sums, pairs = spread1.merged(True)
    tell(1, message(plan, [(0, first_sums), (1, second_sums), (2, third_sums), (3, pairs)]))

    def settle(m, ref):
        hear(m)
        for d in range(count):
            for l in range(plan.lv):
                at = REG * ORDER.index(d // plan.nc * plan.lv + l) + d % plan.nc * plan.cw
                ref[at : at + plan.cw, :] = gat[m, d, l * plan.cw : (l + 1) * plan.cw, :]

    def last_message():
        last_pairs, last_sums = spread2.merged()
        value = message(plan, [(0, last_pairs), (3, last_sums)])
        sub, block = iota((8, LANES), 0), iota((8, LANES), 1) // BLOCK
        for k in range(4):
            value = jnp.where((sub == k) & (block == 1), rolled(dots, BLOCK * (1 - k), 1), value)
        tell(2, value)

    settle(0, q0)
    inverse = whole_inverse(coarse_matrix(q0[...], BLOCK), last_message)
    c0 = same(dot(inverse, q0[...]), 0)
    settle(1, q1)

    def over(value):
        return jnp.sum(value, axis=0, keepdims=True)

    regions = c0.shape[0]
    block = iota((regions, LANES), 1) // BLOCK
    start = 3 * BLOCK + jnp.where(block == 3, 0, 9 * block)
    for k in range(9):
        diag[k] = taken(q1[...], start + k)
    for ref in (cpad, cpad1):
        ref[...] = jnp.zeros_like(ref)
    cpad[8 : 8 + regions, :] = c0
    reduced = q1[...] - banded(diag, cpad)
    solved = dot(inverse, reduced)
    c1, e2 = same(solved, 0), same(solved, 1)
    cpad1[8 : 8 + regions, :] = c1
    image = banded(diag, cpad1)
    in_c1 = over(c1 * reduced)
    image_c1 = over(c1 * image)
    turned = same(dot(inverse, image), 0)
    settle(2, q2)
    for k in range(9):
        diag[k] = jnp.broadcast_to(q2[:, k : k + 1], (regions, LANES))
    mixed = jnp.where(block == 3, 2.0 * q2[...] - banded(diag, cpad), q1[...] + reduced)
    all_dots = jnp.sum(gat[2], axis=0)
    row_block = iota((1, LANES), 1) // BLOCK
    dots = -over(c0 * mixed)
    for k in range(4):
        dots = dots + jnp.where(row_block == k, rolled(all_dots[k : k + 1], BLOCK * (k - 1), 1), 0.0)
    rho, m1, m2, m3 = [same(dots, k) for k in range(4)]
    with_s1, with_s2, with_s3 = [same(in_c1, k) for k in range(3)]
    curve = m1 - with_s1
    alpha = rho / curve
    square = m2 - 2.0 * with_s2 + same(image_c1, 0)
    c2 = c1 - alpha * (e2 - turned)
    now = reduced - alpha * (pltpu.roll(reduced, 3 * BLOCK, 1) - image)
    in_c2 = same(over(c2 * now), 0)
    image_dot = m1 - 2.0 * alpha * (m2 - with_s2) + alpha * alpha * (m3 - 2.0 * with_s3 + same(image_c1, 1))
    rho1 = rho - 2.0 * alpha * curve + alpha * alpha * square
    beta = rho1 / rho
    curve1 = image_dot - in_c2 + 2.0 * beta * (curve - alpha * square) + beta * beta * curve
    alpha1 = rho1 / curve1
    mix = alpha + alpha1 * beta
    kappa, lam = mix + alpha1, alpha * alpha1
    coefs = jnp.where(block == 0, c0 - mix * c1 - alpha1 * c2, jnp.where(block == 1, lam * c1 - kappa * c0, lam * c0))
    scales = 6 * plan.levels * n
    cx_ref[scales : scales + n, :] = wide(kappa)
    cx_ref[scales + n : scales + 2 * n, :] = wide(lam)

    knat[...] = jnp.zeros_like(knat)
    for q in range(REG):
        at = REG * (1 + ORDER[q])
        knat[at : at + REG, :] = coefs[q * REG : (q + 1) * REG]
    near = knat[pl.ds(pl.multiple_of(r * (plan.lv * REG), REG), LANES), :].T
    base = c * plan.cw - 1 + (iota((3 * BLOCK, cols), 1) + plan.width // 2) // plan.width
    for b in (0, 1):
        column = jnp.clip(base + b, 0, REG - 1)
        for l in range(plan.levels):
            value = taken(near[: 3 * BLOCK], column + l * REG)
            for f in range(3):
                at = ((2 * f + b) * plan.levels + l) * n
                cx_ref[at : at + n, :] = value[f * BLOCK : f * BLOCK + n]

    out3 = pltpu.make_async_copy(cx_ref, cx_out, out_sem.at[3])
    out3.start()
    out0.wait()
    out1.wait()
    out2.wait()
    out3.wait()
    legs.sent(next_edges)
    for gone in field_edges:
        legs.sent(gone)


def last_kernel(
    plan, b_hbm, b1_hbm, b2_hbm, planes_hbm, cx_hbm, x_hbm, r_hbm,
    braw, b1, b2, planes, xs, rs, cx_ref, in_sem, out_sem, cx_sem,
):
    n, hn = plan.loads, plan.half
    flat_b = braw.reshape(n * plan.pitch, plan.cols)
    flat_x = xs.reshape(n * plan.pitch, plan.cols)
    flat_r = rs.reshape(n * plan.pitch, plan.cols)
    arrivals, departures = [], []
    spread_copy = pltpu.make_async_copy(cx_hbm, cx_ref, cx_sem)
    spread_copy.start()
    pieces = list(plan.pieces())
    for part, (owner, first, last) in enumerate(pieces):
        here, flat = pl.ds(first, last - first), pl.ds(first * n, (last - first) * n)
        arrivals.append([
            pltpu.make_async_copy(src, dst, in_sem.at[part, k])
            for k, (src, dst) in enumerate((
                (planes_hbm.at[:, here], planes.at[:, here]),
                (b_hbm.at[:, here], braw.at[:, here]),
                (b1_hbm.at[flat], b1.at[flat]),
                (b2_hbm.at[flat], b2.at[flat]),
            ))
        ])
        departures.append([
            pltpu.make_async_copy(xs.at[:, here], x_hbm.at[:, here], out_sem.at[part, 0]),
            pltpu.make_async_copy(rs.at[:, here], r_hbm.at[:, here], out_sem.at[part, 1]),
        ])
    for copies in arrivals[:2]:
        for copy in copies:
            copy.start()
    spread_copy.wait()
    scales = 6 * plan.levels * n
    for part, (owner, first, last) in enumerate(pieces):
        for copy in arrivals[part]:
            copy.wait()
        for copies in arrivals[2:] if part == 0 else ():
            for copy in copies:
                copy.start()
        for h in (0, 1):
            kappa, lam = [cx_ref[scales + k * n + h * hn : scales + k * n + (h + 1) * hn, :] for k in (0, 1)]
            cx = []
            for f in range(3):
                for a in (0, 1):
                    for b in (0, 1):
                        at = ((2 * f + b) * plan.levels + owner + a) * n + h * hn
                        cx.append(cx_ref[at : at + hn, :])

            def step(k, u, carry):
                at = pl.ds(pl.multiple_of(k * n + h * hn, 8), hn)
                to = pl.ds(k + h * hn * plan.pitch, hn, stride=plan.pitch)
                v0, v1, v2 = flat_b[to, :], b1[at, :], b2[at, :]
                x = kappa * v0 - lam * v1
                r = v0 - kappa * v1 + lam * v2
                plain = None
                for m in range(4):
                    w0 = row_of(planes, W0 + m, k)
                    w1 = row_of(planes, W1 + m, k)
                    x = x + w0 * cx[4 + m] + w1 * cx[8 + m]
                    r = r - w0 * cx[m] - w1 * cx[4 + m] - row_of(planes, W2 + m, k) * cx[8 + m]
                    term = row_of(planes, Z + m, k) * cx[m]
                    plain = term if plain is None else plain + term
                flat_x[to, :] = row_of(planes, MINV, k) * x + plain
                flat_r[to, :] = r
                return carry

            over_rows(first, last, step, 0, 4)
        for copy in departures[part]:
            copy.start()
    for copies in departures:
        for copy in copies:
            copy.wait()


def body(load_currents, labels, bump_height, horizontal_class, vertical_class, pad_class, edge_table, pad_table):
    rows, cols = labels.shape
    loads = load_currents.shape[0]
    nr, nc = lax.axis_size("row"), lax.axis_size("col")
    height, width = nr * rows // REG, nc * cols // REG
    plan = Plan(rows, cols, loads, height, width, nr, nc)
    n, regions, count = loads, REG * REG, plan.count
    field = (rows * n, cols)
    tall = ((rows + 2) * n, cols)
    edge = (4, 8, cols)
    sums = (2, LANES, cols)
    spread = (6 * plan.levels * n + 2 * n, cols)

    def vm(*dims):
        return pltpu.VMEM(dims, F32)

    def whole(*dims):
        return pltpu.VMEM(dims, jnp.int32)

    def sm(dims):
        return pltpu.SMEM(dims, F32)

    def dma(*dims):
        return pltpu.SemaphoreType.DMA(dims)

    legs = 4 * 6 + 3 * 8
    b1, b2, planes, cx = pl.pallas_call(
        functools.partial(front_kernel, plan),
        out_shape=(shape(*field), shape(*field), shape(KEPT, rows, cols), shape(*spread)),
        in_specs=[HBM] * 8,
        out_specs=(HBM,) * 4,
        scratch_shapes=[
            whole(rows, cols), whole(rows, cols), whole(rows, cols), vm(rows, cols), whole(rows, cols), sm(edge_table.shape), sm(pad_table.shape),
            vm(n * plan.pitch, cols), vm(*field), vm(*tall), vm(*tall), vm(*field), vm(*field), vm(PLANES, rows, cols),
            vm(*edge), vm(*edge), vm(*edge), vm(*edge), vm(*edge), vm(*edge),
            vm(2, n, cols), vm(2, n, cols), vm(2, n, cols), vm(2, n, cols), vm(2, n, cols), vm(*field),
        ] + [vm(*sums)] * 8 + [
            vm(LANES, LANES),
            vm(2, 8, LANES), vm(4, 8, LANES), vm(2, 8, LANES), vm(2, 8, LANES), vm(2, 8, LANES), vm(2, 8, LANES),
            vm(2, 2, 8, LANES), vm(2, 4, 8, LANES), vm(2, 2, 8, LANES), vm(6, 8, LANES), vm(6, 8, LANES), vm(6, 8, LANES),
            vm(3, 8, LANES), vm(3, count, 8, LANES), vm(regions, LANES), vm(regions, LANES), vm(regions, LANES),
            vm(regions + 16, LANES), vm(regions + 16, LANES), vm(9, regions, LANES), vm(regions + LANES + 2 * REG, LANES), vm(*spread),
            pltpu.SemaphoreType.DMA, dma(7), dma(4), dma(20), dma(legs), dma(3), dma(3),
        ],
        compiler_params=pltpu.CompilerParams(collective_id=0, has_side_effects=True, vmem_limit_bytes=56 * 1024 * 1024),
    )(load_currents.reshape(n * rows, cols), horizontal_class, vertical_class, labels, bump_height, pad_class, edge_table, pad_table)
    staged = (n, plan.pitch, cols)
    return pl.pallas_call(
        functools.partial(last_kernel, plan),
        out_shape=(shape(n, rows, cols),) * 2,
        in_specs=[HBM] * 5,
        out_specs=(HBM, HBM),
        scratch_shapes=[
            vm(*staged), vm(*field), vm(*field), vm(KEPT, rows, cols), vm(*staged), vm(*staged), vm(*spread),
            dma(plan.parts + 2, 4), dma(plan.parts + 2, 2), pltpu.SemaphoreType.DMA,
        ],
        compiler_params=pltpu.CompilerParams(vmem_limit_bytes=56 * 1024 * 1024),
    )(load_currents, b1, b2, planes, cx)


def solution(mesh):
    grid = P("row", "col")
    cube = P(None, "row", "col")
    return jax.shard_map(
        body,
        mesh=mesh,
        in_specs=(cube, grid, grid, grid, grid, grid, P(), P()),
        out_specs=(cube, cube),
        check_vma=False,
    )
```

```python
import functools

import jax
import jax.numpy as jnp
from jax import lax
from jax.experimental import pallas as pl
from jax.experimental.pallas import tpu as pltpu
from jax.sharding import PartitionSpec as P

REG = 16
F32 = jnp.float32
HBM = pl.BlockSpec(memory_space=pltpu.HBM)
BLOCK = 32
LANES = 4 * BLOCK
PITCH = 8
GROUP = 32
MINV, Z, W0, W1, W2, V0, V1, CO = 0, 1, 5, 9, 13, 17, 21, 25
KEPT, PLANES = 17, 33
RIGHT_IN, LEFT_IN, OUTER = 30, 31, 32
ORDER = (0, 2, 4, 6, 8, 10, 12, 14, 1, 5, 9, 13, 3, 11, 7, 15)


def shape(*dims):
    return jax.ShapeDtypeStruct(dims, F32)


def iota(dims, axis):
    return lax.broadcasted_iota(jnp.int32, dims, axis)


def rolled(value, shift, axis):
    shift = shift % value.shape[axis]
    return pltpu.roll(value, shift, axis) if shift else value


class Plan:
    def __init__(self, rows, cols, loads, height, width, row_devices, col_devices):
        self.rows, self.cols, self.loads = rows, cols, loads
        self.height, self.width = height, width
        self.nr, self.nc = row_devices, col_devices
        self.count = row_devices * col_devices
        self.lv, self.cw = rows // height, cols // width
        self.parts = self.lv + 1
        self.levels = self.lv + 2
        self.half = loads // 2
        self.pitch = rows + PITCH

    def chunks(self):
        half = self.height // 2
        for part in range(self.parts):
            yield part, max(0, part * self.height - half), min(self.rows, part * self.height + half)

    def reached(self, part, first, last):
        reach, middle = self.height // 4 + 3, part * self.height
        low, high = (middle - reach) // 4 * 4, -(-(middle + reach) // 4) * 4
        spans = ((first, min(last, low), (0, 1)), (max(first, low), min(last, high), (0, 1, 2, 3)), (max(first, high), last, (2, 3)))
        return [span for span in spans if span[1] > span[0]]

    def pieces(self):
        for part, first, last in self.chunks():
            cut = first + 8 if part == 0 else last - 8 if part == self.parts - 1 else first
            for start, stop in ((first, cut), (cut, last)):
                if stop > start:
                    yield part, start, stop


def over_rows(first, last, step, init, group=4):
    def body(g, carry):
        for u in range(group):
            carry = step(first + g * group + u, u, carry)
        return carry

    return lax.fori_loop(0, (last - first) // group, body, init)


def over_groups(first, last, group, init, size=8):
    return lax.fori_loop(0, (last - first) // size, lambda g, carry: group(first + g * size, carry), init)


def row_of(ref, k, i):
    return ref[k, pl.ds(i, 1), :]


class Legs:
    def __init__(self, plan, send_sem, recv_sem):
        self.plan, self.send_sem, self.recv_sem = plan, send_sem, recv_sem
        self.used = 0
        self.r, self.c = lax.axis_index("row"), lax.axis_index("col")

    def inside(self, dr, dc):
        r, c = self.r + dr, self.c + dc
        return (r >= 0) & (r < self.plan.nr) & (c >= 0) & (c < self.plan.nc)

    def make(self, items, sends):
        out = []
        for dr, dc, src, dst in items:
            target = (lax.rem(self.r + dr + self.plan.nr, self.plan.nr), lax.rem(self.c + dc + self.plan.nc, self.plan.nc))
            copy = pltpu.make_async_remote_copy(
                src_ref=src,
                dst_ref=dst,
                send_sem=self.send_sem.at[sends + len(out)],
                recv_sem=self.recv_sem.at[self.used],
                device_id=target,
                device_id_type=pl.DeviceIdType.MESH,
            )
            self.used += 1
            out.append((self.inside(dr, dc), self.inside(-dr, -dc), copy))
        return out

    def start(self, legs):
        for goes, _, copy in legs:
            pl.when(goes)(copy.start)

    def wait(self, legs):
        for _, comes, copy in legs:
            pl.when(comes)(copy.wait_recv)

    def sent(self, legs):
        for goes, _, copy in legs:
            pl.when(goes)(copy.wait_send)


def beside(src, dst):
    return [(1, 0, src.at[0], dst.at[0]), (-1, 0, src.at[1], dst.at[1]), (0, 1, src.at[2], dst.at[2]), (0, -1, src.at[3], dst.at[3])]


def looked_up(table_ref, classes):
    out = jnp.zeros(classes.shape, F32)
    for k in range(table_ref.shape[0]):
        out = jnp.where(classes == k, table_ref[k], out)
    return out


def put_edges(ref, k, value, row_end=True):
    rows, cols = value.shape
    ref[0, k : k + 1, :] = value[rows - 1 :]
    ref[1, k : k + 1, :] = value[:1]
    turned = value.T
    ref[2, k : k + 1, :] = turned[cols - 1 :]
    ref[3, k : k + 1, :] = turned[:1]


class Around:
    def __init__(self, edge_ref, rows, cols):
        self.edge_ref, self.rows, self.cols = edge_ref, rows, cols
        self.i, self.j = iota((rows, cols), 0), iota((rows, cols), 1)

    def column(self, side, k):
        return jnp.broadcast_to(self.edge_ref[side, k : k + 1, :], (self.cols, self.rows)).T

    def left(self, value, k):
        return jnp.where(self.j == 0, self.column(2, k), pltpu.roll(value, 1, 1))

    def right(self, value, k):
        return jnp.where(self.j == self.cols - 1, self.column(3, k), pltpu.roll(value, self.cols - 1, 1))

    def top(self, value, k):
        return jnp.where(self.i == 0, self.edge_ref[0, k : k + 1, :], pltpu.roll(value, 1, 0))

    def low(self, value, k):
        return jnp.where(self.i == self.rows - 1, self.edge_ref[1, k : k + 1, :], pltpu.roll(value, self.rows - 1, 0))

    def turns(self, at, size, step):
        out = None
        for p in range(1, size // step + 1):
            hit = at == p * step - step // 2
            out = hit if out is None else out | hit
        return out

    def images(self, plan, planes, source, k):
        values = [planes[source + m] for m in range(4)]
        to_right = self.turns(self.j + 1, plan.cols, plan.width)
        to_left = self.turns(self.j, plan.cols, plan.width)
        to_low = self.turns(self.i + 1, plan.rows, plan.height)
        to_top = self.turns(self.i, plan.rows, plan.height)

        def shifted(reader, turn, step, later):
            seen = [reader(value, k + m) for m, value in enumerate(values)]
            out = list(seen)
            for m in range(4):
                if bool(m & step) == later:
                    out[m] = jnp.where(turn, seen[m ^ step], seen[m])
                else:
                    out[m] = jnp.where(turn, 0.0, seen[m])
            return out

        right = shifted(self.right, to_right, 1, True)
        left = shifted(self.left, to_left, 1, False)
        low = shifted(self.low, to_low, 2, True)
        top = shifted(self.top, to_top, 2, False)
        return [
            planes[CO] * values[m]
            - planes[CO + 1] * right[m]
            - planes[CO + 2] * left[m]
            - planes[CO + 3] * low[m]
            - planes[CO + 4] * top[m]
            for m in range(4)
        ]


def windows(plan):
    rows, cols = plan.rows, plan.cols
    i, j = iota((rows, cols), 0), iota((rows, cols), 1)
    base_row = jnp.zeros((rows, cols), F32) + (lax.axis_index("row") * plan.lv - 1).astype(F32)
    base_col = jnp.zeros((rows, cols), F32) + (lax.axis_index("col") * plan.cw - 1).astype(F32)
    for p in range(1, plan.parts):
        base_row = base_row + jnp.where(i >= p * plan.height - plan.height // 2, 1.0, 0.0)
    for p in range(1, plan.cw + 1):
        base_col = base_col + jnp.where(j >= p * plan.width - plan.width // 2, 1.0, 0.0)
    return base_row, base_col


def hits_of(label, base_row, base_col):
    high = jnp.floor(label * (1.0 / REG))
    a, b = high - base_row, label - REG * high - base_col
    return [(a == m) & (b == n) for m in (0.0, 1.0) for n in (0.0, 1.0)]


def add_sums(plan, s_ref, h, part, acc):
    n, hn = plan.loads, plan.half
    for a in (0, 1):
        for b in (0, 1):
            at = (part + a) * n + h * hn
            s_ref[b, at : at + hn, :] = s_ref[b, at : at + hn, :] + acc[2 * a + b]


def packed(plan, s_ref):
    out = [None] * (plan.cw + 2)
    half = plan.width // 2
    for b in (0, 1):
        turned = s_ref[b].T
        for g in range(plan.cw + 1):
            part = turned[max(0, g * plan.width - half) : min(plan.cols, g * plan.width + half)]
            term = jnp.sum(part, axis=0, keepdims=True)
            out[g + b] = term if out[g + b] is None else out[g + b] + term
    out.append(jnp.zeros((8 - len(out), LANES), F32))
    return jnp.concatenate(out, axis=0)


def pair_sums(plan, planes, x, y, pair_ref, q):
    terms = {}
    for part, first, last in plan.chunks():
        for k in range(4):
            for m in range(4):
                da, db = m // 2 - k // 2, m % 2 - k % 2
                at = (k % 2, (part + k // 2) * BLOCK + q + (da + 1) * 3 + db + 1)
                term = jnp.sum(planes[x + k, first:last, :] * planes[y + m, first:last, :], axis=0, keepdims=True)
                terms[at] = term if at not in terms else terms[at] + term
    for (b, at), term in terms.items():
        pair_ref[b, at : at + 1, :] = term


class Spread:
    def __init__(self, plan, legs, planes, sides, got_planes, got_sides):
        self.plan, self.planes, self.sides = plan, planes, sides
        self.got_planes, self.got_sides = got_planes, got_sides
        west, east = sides.at[0], sides.at[1]
        self.legs = legs
        self.mine = legs.make([
            (1, 0, planes, got_planes.at[0]),
            (-1, 0, planes, got_planes.at[1]),
            (0, -1, west, got_sides.at[0]),
            (1, -1, west, got_sides.at[1]),
            (-1, -1, west, got_sides.at[2]),
            (0, 1, east, got_sides.at[3]),
            (1, 1, east, got_sides.at[4]),
            (-1, 1, east, got_sides.at[5]),
        ], 12)

    def send(self, values):
        last = self.plan.cw + 1
        for k, value in enumerate(values):
            self.planes[k] = value
            self.sides[0, k : k + 1, :] = value[:1]
            self.sides[1, k : k + 1, :] = value[last : last + 1]
        self.legs.start(self.mine)

    def meet(self, own, above, below):
        lv = self.plan.lv
        block = iota(own.shape, len(own.shape) - 1) // BLOCK
        shift = lv * BLOCK
        return own + jnp.where(block == 1, rolled(above, -shift, 1), 0.0) + jnp.where(block == lv, rolled(below, shift, 1), 0.0)

    def merged(self, early=False):
        self.legs.wait(self.mine)
        if not early:
            self.legs.sent(self.mine)
        sub = iota((8, LANES), 0)
        sides = self.got_sides
        right = self.meet(sides[0], sides[1], sides[2])
        left = self.meet(sides[3], sides[4], sides[5])
        out = []
        for k in range(self.planes.shape[0]):
            value = self.meet(self.planes[k], self.got_planes[0, k], self.got_planes[1, k])
            value = value + jnp.where(sub == self.plan.cw, right[k : k + 1], 0.0) + jnp.where(sub == 1, left[k : k + 1], 0.0)
            out.append(value)
        return out


def message(plan, pieces):
    sub, block = iota((8, LANES), 0), iota((8, LANES), 1) // BLOCK
    out = jnp.zeros((8, LANES), F32)
    for spot, value in pieces:
        for l in range(plan.lv):
            first = l * plan.cw
            moved = rolled(rolled(value, first - 1, 0), BLOCK * (spot - 1 - l), 1)
            out = jnp.where((block == spot) & (sub >= first) & (sub < first + plan.cw), moved, out)
    return out


def fold(value):
    half = value + pltpu.roll(value, 2 * BLOCK, 1)
    return half + pltpu.roll(half, BLOCK, 1)


def same(value, spot):
    return fold(jnp.where(iota(value.shape, 1) // BLOCK == spot, value, 0.0))


def halves(value):
    high = value.astype(jnp.bfloat16)
    return high, (value - high.astype(F32)).astype(jnp.bfloat16)


def dot(a, b, contract=((1,), (0,))):
    (a_high, a_low), (b_high, b_low) = halves(a), halves(b)
    total = None
    for left, right in ((a_high, b_low), (a_low, b_high), (a_high, b_high)):
        term = lax.dot_general(left, right, (contract, ((), ())), preferred_element_type=F32)
        total = term if total is None else total + term
    return total


def taken(value, index):
    return jnp.take_along_axis(value, index, axis=1, mode="promise_in_bounds")


def small_inverses(value):
    lane, sub = iota(value.shape, 1), iota(value.shape, 0)
    start = lane // REG * REG
    cols = [taken(value, start + j) for j in range(REG)]
    for k in range(REG):
        col = cols[k]
        here = sub == k
        recip = 1.0 / col[k : k + 1]
        left = jnp.where(here, -1.0, col)
        for j in range(REG):
            if j != k:
                row = cols[j][k : k + 1] * recip
                cols[j] = jnp.where(here, 0.0, cols[j]) - left * row
        cols[k] = jnp.where(here, recip, -col * recip)
    out = cols[0]
    for j in range(1, REG):
        out = jnp.where(lane % REG == j, cols[j], out)
    return out


def block_inverses(matrix, first, count):
    width = matrix.shape[1]
    lane, sub = iota((REG, width), 1), iota((REG, width), 0)
    value = jnp.where(lane % REG == sub, 1.0, 0.0)
    for q in range(first, first + count):
        value = jnp.where(lane // REG == q, matrix[q * REG : (q + 1) * REG], value)
    value = small_inverses(value)
    return jnp.concatenate([jnp.where(lane // REG == q, value, 0.0) for q in range(first, first + count)], axis=0)


def placed(value, first, total):
    pieces = []
    if first:
        pieces.append(jnp.zeros((first, value.shape[1]), F32))
    pieces.append(value)
    rest = total - first - value.shape[0]
    if rest:
        pieces.append(jnp.zeros((rest, value.shape[1]), F32))
    return jnp.concatenate(pieces, axis=0) if len(pieces) > 1 else value


def tail_inverse(matrix, first, count, between):
    size = matrix.shape[0]
    if count == 1:
        return block_inverses(matrix, first, 1)
    a, b, c = first * REG, (first + count // 2) * REG, (first + count) * REG
    lane = iota((1, size), 1)
    early, late = (lane >= a) & (lane < b), (lane >= b) & (lane < c)
    x = block_inverses(matrix, first, count // 2)
    f = placed(jnp.where(late, matrix[a:b], 0.0), a, size)
    y = dot(x, f)
    y_full = placed(y, a, size)
    rest = matrix[b:c] - dot(jnp.where(early, matrix[b:c], 0.0), y_full)
    rest = jnp.where(late, rest, 0.0)
    if count == 2:
        between()
    inner = tail_inverse(placed(rest, b, size), first + count // 2, count // 2, between)
    t = dot(y, placed(inner, b, size))
    top = jnp.where(early, x + dot(t, y_full, ((1,), (1,))), -t)
    turned = placed(t, a, size).T
    low = jnp.where(early, -turned[b:c], inner)
    return jnp.concatenate([top, low], axis=0)


def whole_inverse(matrix, between):
    half = matrix.shape[0] // 2
    x = block_inverses(matrix[:half, :half], 0, half // REG)
    y = dot(x, matrix[:half, half:])
    rest = matrix[half:, half:] - dot(matrix[half:, :half], y)
    inner = tail_inverse(rest, 0, half // REG, between)
    t = dot(y, inner)
    top = jnp.concatenate([x + dot(t, y, ((1,), (1,))), -t], axis=1)
    return jnp.concatenate([top, jnp.concatenate([-t.T, inner], axis=1)], axis=0)


def region_of(at):
    q = at // REG
    row = jnp.where(q < 8, 2 * q, jnp.where(q < 12, 4 * q - 31, jnp.where(q < 14, 8 * q - 93, jnp.where(q < 15, 7, 15))))
    return row * REG + at % REG


def coarse_matrix(value, first):
    size = value.shape[0]
    gap = region_of(iota((size, size), 1)) - region_of(iota((size, size), 0))
    total = jnp.zeros((size, size), F32)
    for k in range(9):
        total = jnp.where(gap == REG * (k // 3 - 1) + k % 3 - 1, value[:, first + k : first + k + 1], total)
    return total


def banded(diag_ref, pad_ref):
    out = []
    for q in range(REG):
        total = None
        for k in range(9):
            row = ORDER[q] + k // 3 - 1
            if 0 <= row < REG:
                at = 8 + REG * ORDER.index(row) + k % 3 - 1
                term = diag_ref[k, q * REG : (q + 1) * REG, :] * pad_ref[at : at + REG, :]
                total = term if total is None else total + term
        out.append(total)
    return jnp.concatenate(out, axis=0)


def wide(value):
    return jnp.broadcast_to(value, (LANES, LANES)).T[:BLOCK]


def front_kernel(
    plan, b_hbm, h_hbm, v_hbm, label_hbm, bump_hbm, pad_class_hbm, edge_hbm, pad_hbm,
    bt_out, b1_out, b2_out, planes_out, cx_out,
    h_ref, v_ref, label_ref, bump_ref, pad_class_ref, edge_table, pad_table, braw, bt, u0, u1, b1, b2, planes, ea, eb, ec, ga, gb, gc, brow, bcol, ccol, cpack, cpack1, beyond,
    s0, s1, s2, s3, s4, pa, pb, pc, tacc,
    set0, set1, set2, side0, side1, side2, gset0, gset1, gset2, gside0, gside1, gside2,
    note, gat, q0, q1, q2, cpad, cpad1, diag, knat, cx_ref,
    in_sem, small_sem, out_sem, send_sem, recv_sem, note_send, note_recv,
):
    rows, cols, n, hn = plan.rows, plan.cols, plan.loads, plan.half
    r, c = lax.axis_index("row"), lax.axis_index("col")
    me = r * plan.nc + c
    count = plan.count
    barrier = pltpu.get_barrier_semaphore()

    def device(d):
        other = lax.rem(me + d, count)
        return (other // plan.nc, lax.rem(other, plan.nc))

    def fetch(k):
        here, there = pl.ds(pl.multiple_of(k * rows, 8), rows), pl.ds(pl.multiple_of(k * plan.pitch, 8), rows)
        return pltpu.make_async_copy(b_hbm.at[here], braw.at[there], in_sem)

    def fetch_start(k, carry):
        fetch(k).start()
        return carry

    small = [
        pltpu.make_async_copy(src, dst, small_sem.at[k])
        for k, (src, dst) in enumerate((
            (h_hbm, h_ref), (edge_hbm, edge_table), (v_hbm, v_ref), (label_hbm, label_ref),
            (bump_hbm, bump_ref), (pad_class_hbm, pad_class_ref), (pad_hbm, pad_table),
        ))
    ]
    for copy in small:
        copy.start()
    lax.fori_loop(0, n, fetch_start, 0)
    for ref in (ga, gb, gc, brow, bcol, ccol, gset0, gset1, gset2, gside0, gside1, gside2):
        ref[...] = jnp.zeros_like(ref)
    u1[0:n, :] = jnp.zeros((n, cols), F32)
    u1[(rows + 1) * n :, :] = jnp.zeros((n, cols), F32)

    def greet(d, carry):
        pl.semaphore_signal(barrier, inc=1, device_id=device(d), device_id_type=pl.DeviceIdType.MESH)
        return carry

    lax.fori_loop(1, count, greet, 0)

    for copy in small:
        copy.wait()
    i, j = iota((rows, cols), 0), iota((rows, cols), 1)
    row_end = jnp.where(r == plan.nr - 1, rows - 1, rows)
    col_end = jnp.where(c == plan.nc - 1, cols - 1, cols)
    planes[CO + 1] = jnp.where(j == col_end, 0.0, looked_up(edge_table, h_ref[...]))
    planes[CO + 3] = jnp.where(i == row_end, 0.0, looked_up(edge_table, v_ref[...]))
    for ref in (ea, eb, ec):
        ref[...] = jnp.zeros_like(ref)
    put_edges(ea, 0, label_ref[...].astype(F32))
    put_edges(ea, 1, bump_ref[...])
    put_edges(ea, 2, planes[CO + 1])
    put_edges(ea, 3, planes[CO + 3])
    legs = Legs(plan, send_sem, recv_sem)
    first_edges = legs.make(beside(ea, ga), 0)
    base_row, base_col = windows(plan)
    bump = bump_ref[...]
    for k, hit in enumerate(hits_of(label_ref[...].astype(F32), base_row, base_col)):
        planes[Z + k] = jnp.where(hit, bump, 0.0)
    pl.semaphore_wait(barrier, count - 1)
    legs.start(first_edges)

    for ref in (s0, s1, s2, s3, s4, pa, pb, pc):
        ref[...] = jnp.zeros_like(ref)
    pltpu.make_async_copy(b_hbm, braw.at[pl.ds(0, n * rows)], in_sem).wait()

    lane = iota((hn, cols), 1)
    even = lane % 2 == 0
    zero = jnp.zeros((hn, cols), F32)

    def own(h):
        return slice(h * hn, (h + 1) * hn)

    def spot(h, k):
        return pl.ds(pl.multiple_of(k * n + h * hn, 8), hn)

    def keep_ends(ref, h, field, skip):
        pack, top = [zero, zero], None
        for k in range(rows):
            moved = rolled(field[spot(h, k + skip), :], k, 1)
            top = moved if k == 0 else top
            pack[k % 2] = moved if k < 2 else jnp.where(lane >= k - 1, moved, pack[k % 2])
        pack[0] = jnp.where(lane == cols - 1, top, pack[0])
        ref[0, own(h), :] = jnp.where(even, pack[1], pack[0])
        ref[1, own(h), :] = jnp.where(even, pack[0], pack[1])

    def halo_rows(h, from_left, from_right):
        from_left = -ga[2, 2:3, :] * from_left
        from_right = pltpu.roll(-ea[2, 2:3, :] * from_right, cols - 1, 1)
        pair = [jnp.where(even, from_left, from_right), jnp.where(even, from_right, from_left)]
        outer = (lane == 0) | (lane == cols - 1)
        for k in range(rows):
            beyond[spot(h, k), :] = jnp.where(outer, rolled(pair[k % 2], -k, 1), 0.0)

    for h in (0, 1):
        for part, first, last in plan.chunks():

            def group(base, acc):
                for u in range(8):
                    k = base + u
                    v = braw[pl.ds(k + h * hn * plan.pitch, hn, stride=plan.pitch), :]
                    bt[spot(h, k), :] = v
                    acc = tuple(x + row_of(planes, Z + m, k) * v for m, x in enumerate(acc))
                return acc

            add_sums(plan, s0, h, part, over_groups(first, last, group, (zero,) * 4))
        keep_ends(cpack, h, bt, 0)
    load_edges = legs.make([
        (1, 0, bt.at[pl.ds((rows - 1) * n, n)], brow.at[0]),
        (-1, 0, bt.at[pl.ds(0, n)], brow.at[1]),
        (0, 1, cpack.at[0], bcol.at[0]),
        (0, -1, cpack.at[1], bcol.at[1]),
    ], 4)
    legs.start(load_edges)
    out4 = pltpu.make_async_copy(bt, bt_out, out_sem.at[4])
    out4.start()

    legs.wait(first_edges)
    around = Around(ga, rows, cols)
    right, down = planes[CO + 1], planes[CO + 3]
    left, upper = around.left(right, 2), around.top(down, 3)
    diagonal = looked_up(pad_table, pad_class_ref[...]) + right + left + down + upper
    minv = 1.0 / diagonal
    planes[CO] = diagonal
    planes[CO + 2] = left
    planes[RIGHT_IN] = jnp.where(j == cols - 1, 0.0, right)
    planes[LEFT_IN] = jnp.where(j == 0, 0.0, left)
    planes[CO + 4] = upper
    planes[MINV] = minv
    named = label_ref[...].astype(F32)
    bump = bump_ref[...]
    total = None
    for label, weight in (
        (named, diagonal * bump),
        (around.right(named, 0), -right * around.right(bump, 1)),
        (around.left(named, 0), -left * around.left(bump, 1)),
        (around.low(named, 0), -down * around.low(bump, 1)),
        (around.top(named, 0), -upper * around.top(bump, 1)),
    ):
        terms = [jnp.where(hit, weight, 0.0) for hit in hits_of(label, base_row, base_col)]
        total = terms if total is None else [t + u for t, u in zip(total, terms)]
    put_edges(eb, 0, minv)
    for k in range(4):
        planes[W0 + k] = total[k]
        value = total[k] * minv
        planes[V0 + k] = value
        put_edges(eb, 1 + k, value)
    image_edges = legs.make(beside(eb, gb), 8)
    legs.start(image_edges)

    pair_sums(plan, planes, Z, W0, pa, 0)
    spread0 = Spread(plan, legs, set0, side0, gset0, gside0)
    spread0.send([packed(plan, s0), packed(plan, pa)])

    for h in (0, 1):
        dots = zero
        for part, first, last in plan.chunks():

            def step(k, u, carry):
                dots, acc = carry
                v = bt[spot(h, k), :]
                w = row_of(planes, MINV, k) * v
                u0[spot(h, k + 1), :] = w
                return dots + v * w, tuple(x + row_of(planes, V0 + m, k) * v for m, x in enumerate(acc))

            dots, acc = over_rows(first, last, step, (dots, (zero,) * 4))
            add_sums(plan, s1, h, part, acc)
        tacc[h * hn : (h + 1) * hn, :] = dots

    def note_copy(m, d):
        return pltpu.make_async_remote_copy(
            src_ref=note.at[m],
            dst_ref=gat.at[m, me],
            send_sem=note_send.at[m],
            recv_sem=note_recv.at[m],
            device_id=device(d),
            device_id_type=pl.DeviceIdType.MESH,
        )

    def tell(m, value):
        note[m] = value
        gat[m, pl.ds(me, 1)] = value[None]

        def go(d, carry):
            note_copy(m, d).start()
            return carry

        lax.fori_loop(1, count, go, 0)

    def hear(m):
        others = gat.at[m, pl.ds(0, count - 1)]
        every = pltpu.make_async_remote_copy(
            src_ref=others,
            dst_ref=others,
            send_sem=note_send.at[m],
            recv_sem=note_recv.at[m],
            device_id=device(1),
            device_id_type=pl.DeviceIdType.MESH,
        )
        every.wait_recv()
        every.wait_send()

    legs.wait(load_edges)
    for h in (0, 1):
        halo_rows(h, pltpu.roll(bcol[0, own(h), :], 1, 1), bcol[1, own(h), :])
    legs.wait(image_edges)
    u0[0:n, :] = brow[0] * gb[0, 0:1, :]
    u0[(rows + 1) * n :, :] = brow[1] * gb[1, 0:1, :]
    around = Around(gb, rows, cols)
    planes[OUTER] = jnp.where(j == 0, around.column(2, 0), around.column(3, 0))
    for k, value in enumerate(around.images(plan, planes, V0, 1)):
        planes[W1 + k] = value
        value = value * planes[MINV]
        planes[V1 + k] = value
        put_edges(ec, k, value)
    for gone in (first_edges, load_edges, image_edges):
        legs.sent(gone)
    next_edges = legs.make(beside(ec, gc), 0)
    legs.start(next_edges)

    def stencil(field, h, k):
        z = field[spot(h, k + 1), :]
        f = (
            row_of(planes, CO, k) * z
            - row_of(planes, RIGHT_IN, k) * pltpu.roll(z, cols - 1, 1)
            - row_of(planes, LEFT_IN, k) * pltpu.roll(z, 1, 1)
            - row_of(planes, CO + 3, k) * field[spot(h, k + 2), :]
            - row_of(planes, CO + 4, k) * field[spot(h, k), :]
        )
        return z, f

    field_edges = []
    for h in (0, 1):
        dots, more = zero, zero
        for part, first, last in plan.chunks():

            def group(base, carry):
                dots, more, acc, bcc = carry
                for u in range(GROUP):
                    k = base + u
                    z, f = stencil(u0, h, k)
                    f = f + row_of(planes, OUTER, k) * beyond[spot(h, k), :]
                    w = row_of(planes, MINV, k) * f
                    b1[spot(h, k), :] = f
                    u1[spot(h, k + 1), :] = w
                    acc = tuple(x + row_of(planes, V0 + m, k) * f for m, x in enumerate(acc))
                    bcc = tuple(x + row_of(planes, V1 + m, k) * f for m, x in enumerate(bcc))
                    dots, more = dots + z * f, more + w * f
                return dots, more, acc, bcc

            dots, more, acc, bcc = over_groups(first, last, group, (dots, more, (zero,) * 4, (zero,) * 4), GROUP)
            add_sums(plan, s2, h, part, acc)
            add_sums(plan, s3, h, part, bcc)
        tacc[n + h * hn : n + (h + 1) * hn, :] = dots
        tacc[2 * n + h * hn : 2 * n + (h + 1) * hn, :] = more
        keep_ends(cpack1, h, u1, 1)
        mine = pl.ds(h * hn, hn)
        field_edges.append(legs.make([
            (1, 0, u1.at[pl.ds(rows * n + h * hn, hn)], u1.at[pl.ds(h * hn, hn)]),
            (-1, 0, u1.at[pl.ds(n + h * hn, hn)], u1.at[pl.ds((rows + 1) * n + h * hn, hn)]),
            (0, 1, cpack1.at[0, mine], ccol.at[0, mine]),
            (0, -1, cpack1.at[1, mine], ccol.at[1, mine]),
        ], 4 + 4 * h))
        legs.start(field_edges[h])
        if h == 0:
            load_sums, energy = spread0.merged()
            tell(0, message(plan, [(0, load_sums), (1, energy)]))
    out1 = pltpu.make_async_copy(b1, b1_out, out_sem.at[0])
    out1.start()

    pair_sums(plan, planes, W0, V0, pb, 0)
    pair_sums(plan, planes, W1, V0, pb, 9)
    pair_sums(plan, planes, W1, V1, pb, 18)
    spread1 = Spread(plan, legs, set1, side1, gset1, gside1)
    spread1.send([packed(plan, s1), packed(plan, s2), packed(plan, s3), packed(plan, pb)])

    legs.wait(next_edges)
    around = Around(gc, rows, cols)
    for k, value in enumerate(around.images(plan, planes, V1, 0)):
        planes[W2 + k] = value
    out0 = pltpu.make_async_copy(planes.at[pl.ds(0, KEPT)], planes_out, out_sem.at[1])
    out0.start()
    for h in (0, 1):
        legs.wait(field_edges[h])
        halo_rows(h, pltpu.roll(ccol[0, own(h), :], 1, 1), ccol[1, own(h), :])
        dots = zero
        for part, first, last in plan.chunks():

            def group(base, carry):
                dots, acc = carry
                for u in range(GROUP):
                    k = base + u
                    z, f = stencil(u1, h, k)
                    f = f + beyond[spot(h, k), :]
                    b2[spot(h, k), :] = f
                    dots = dots + z * f
                    acc = tuple(x + row_of(planes, V1 + m, k) * f for m, x in enumerate(acc))
                return dots, acc

            dots, acc = over_groups(first, last, group, (dots, (zero,) * 4), GROUP)
            add_sums(plan, s4, h, part, acc)
        tacc[3 * n + h * hn : 3 * n + (h + 1) * hn, :] = dots
    out2 = pltpu.make_async_copy(b2, b2_out, out_sem.at[2])
    out2.start()
    pair_sums(plan, planes, W2, V1, pc, 0)
    legs.sent(spread1.mine)
    spread2 = Spread(plan, legs, set2, side2, gset2, gside2)
    spread2.send([packed(plan, pc), packed(plan, s4)])
    dots = jnp.sum(tacc[...].T, axis=0, keepdims=True)

    first_sums, second_sums, third_sums, pairs = spread1.merged(True)
    tell(1, message(plan, [(0, first_sums), (1, second_sums), (2, third_sums), (3, pairs)]))

    def settle(m, ref):
        hear(m)
        for d in range(count):
            for l in range(plan.lv):
                at = REG * ORDER.index(d // plan.nc * plan.lv + l) + d % plan.nc * plan.cw
                ref[at : at + plan.cw, :] = gat[m, d, l * plan.cw : (l + 1) * plan.cw, :]

    def last_message():
        last_pairs, last_sums = spread2.merged()
        value = message(plan, [(0, last_pairs), (3, last_sums)])
        sub, block = iota((8, LANES), 0), iota((8, LANES), 1) // BLOCK
        for k in range(4):
            value = jnp.where((sub == k) & (block == 1), rolled(dots, BLOCK * (1 - k), 1), value)
        tell(2, value)

    settle(0, q0)
    inverse = whole_inverse(coarse_matrix(q0[...], BLOCK), last_message)
    c0 = same(dot(inverse, q0[...]), 0)
    settle(1, q1)

    def over(value):
        return jnp.sum(value, axis=0, keepdims=True)

    regions = c0.shape[0]
    block = iota((regions, LANES), 1) // BLOCK
    start = 3 * BLOCK + jnp.where(block == 3, 0, 9 * block)
    for k in range(9):
        diag[k] = taken(q1[...], start + k)
    for ref in (cpad, cpad1):
        ref[...] = jnp.zeros_like(ref)
    cpad[8 : 8 + regions, :] = c0
    reduced = q1[...] - banded(diag, cpad)
    solved = dot(inverse, reduced)
    c1, e2 = same(solved, 0), same(solved, 1)
    cpad1[8 : 8 + regions, :] = c1
    image = banded(diag, cpad1)
    in_c1 = over(c1 * reduced)
    image_c1 = over(c1 * image)
    turned = same(dot(inverse, image), 0)
    settle(2, q2)
    for k in range(9):
        diag[k] = jnp.broadcast_to(q2[:, k : k + 1], (regions, LANES))
    mixed = jnp.where(block == 3, 2.0 * q2[...] - banded(diag, cpad), q1[...] + reduced)
    all_dots = jnp.sum(gat[2], axis=0)
    row_block = iota((1, LANES), 1) // BLOCK
    dots = -over(c0 * mixed)
    for k in range(4):
        dots = dots + jnp.where(row_block == k, rolled(all_dots[k : k + 1], BLOCK * (k - 1), 1), 0.0)
    rho, m1, m2, m3 = [same(dots, k) for k in range(4)]
    with_s1, with_s2, with_s3 = [same(in_c1, k) for k in range(3)]
    curve = m1 - with_s1
    alpha = rho / curve
    square = m2 - 2.0 * with_s2 + same(image_c1, 0)
    c2 = c1 - alpha * (e2 - turned)
    now = reduced - alpha * (pltpu.roll(reduced, 3 * BLOCK, 1) - image)
    in_c2 = same(over(c2 * now), 0)
    image_dot = m1 - 2.0 * alpha * (m2 - with_s2) + alpha * alpha * (m3 - 2.0 * with_s3 + same(image_c1, 1))
    rho1 = rho - 2.0 * alpha * curve + alpha * alpha * square
    beta = rho1 / rho
    curve1 = image_dot - in_c2 + 2.0 * beta * (curve - alpha * square) + beta * beta * curve
    alpha1 = rho1 / curve1
    mix = alpha + alpha1 * beta
    kappa, lam = mix + alpha1, alpha * alpha1
    coefs = jnp.where(block == 0, c0 - mix * c1 - alpha1 * c2, jnp.where(block == 1, lam * c1 - kappa * c0, lam * c0))
    scales = 6 * plan.levels * n
    cx_ref[scales : scales + n, :] = wide(kappa)
    cx_ref[scales + n : scales + 2 * n, :] = wide(lam)

    knat[...] = jnp.zeros_like(knat)
    for q in range(REG):
        at = REG * (1 + ORDER[q])
        knat[at : at + REG, :] = coefs[q * REG : (q + 1) * REG]
    near = knat[pl.ds(pl.multiple_of(r * (plan.lv * REG), REG), LANES), :].T
    base = c * plan.cw - 1 + (iota((3 * BLOCK, cols), 1) + plan.width // 2) // plan.width
    for b in (0, 1):
        column = jnp.clip(base + b, 0, REG - 1)
        for l in range(plan.levels):
            value = taken(near[: 3 * BLOCK], column + l * REG)
            for f in range(3):
                at = ((2 * f + b) * plan.levels + l) * n
                cx_ref[at : at + n, :] = value[f * BLOCK : f * BLOCK + n]

    out3 = pltpu.make_async_copy(cx_ref, cx_out, out_sem.at[3])
    out3.start()
    out0.wait()
    out1.wait()
    out2.wait()
    out3.wait()
    out4.wait()
    legs.sent(next_edges)
    for gone in field_edges:
        legs.sent(gone)


def last_kernel(
    plan, bt_hbm, b1_hbm, b2_hbm, planes_hbm, cx_hbm, x_hbm, r_hbm,
    bt, b1, b2, planes, xs, rs, cx_ref, in_sem, out_sem, cx_sem,
):
    n, hn = plan.loads, plan.half
    flat_x = xs.reshape(n * plan.pitch, plan.cols)
    flat_r = rs.reshape(n * plan.pitch, plan.cols)
    arrivals, departures = [], []
    spread_copy = pltpu.make_async_copy(cx_hbm, cx_ref, cx_sem)
    spread_copy.start()
    pieces = list(plan.pieces())
    for part, (owner, first, last) in enumerate(pieces):
        here, flat = pl.ds(first, last - first), pl.ds(first * n, (last - first) * n)
        arrivals.append([
            pltpu.make_async_copy(src, dst, in_sem.at[part, k])
            for k, (src, dst) in enumerate((
                (planes_hbm.at[:, here], planes.at[:, here]),
                (bt_hbm.at[flat], bt.at[flat]),
                (b1_hbm.at[flat], b1.at[flat]),
                (b2_hbm.at[flat], b2.at[flat]),
            ))
        ])
        departures.append([
            pltpu.make_async_copy(xs.at[:, here], x_hbm.at[:, here], out_sem.at[part, 0]),
            pltpu.make_async_copy(rs.at[:, here], r_hbm.at[:, here], out_sem.at[part, 1]),
        ])
    for copies in arrivals[:2]:
        for copy in copies:
            copy.start()
    spread_copy.wait()
    scales = 6 * plan.levels * n
    for part, (owner, first, last) in enumerate(pieces):
        for copy in arrivals[part]:
            copy.wait()
        for copies in arrivals[2:] if part == 0 else ():
            for copy in copies:
                copy.start()
        for h in (0, 1):
            kappa, lam = [cx_ref[scales + k * n + h * hn : scales + k * n + (h + 1) * hn, :] for k in (0, 1)]
            cx = []
            for f in range(3):
                for a in (0, 1):
                    for b in (0, 1):
                        at = ((2 * f + b) * plan.levels + owner + a) * n + h * hn
                        cx.append(cx_ref[at : at + hn, :])

            def step(k, u, carry, seen=()):
                at = pl.ds(pl.multiple_of(k * n + h * hn, 8), hn)
                to = pl.ds(k + h * hn * plan.pitch, hn, stride=plan.pitch)
                v0, v1, v2 = bt[at, :], b1[at, :], b2[at, :]
                x = kappa * v0 - lam * v1
                r = v0 - kappa * v1 + lam * v2
                plain = None
                for m in seen:
                    w0 = row_of(planes, W0 + m, k)
                    w1 = row_of(planes, W1 + m, k)
                    x = x + w0 * cx[4 + m] + w1 * cx[8 + m]
                    r = r - w0 * cx[m] - w1 * cx[4 + m] - row_of(planes, W2 + m, k) * cx[8 + m]
                    term = row_of(planes, Z + m, k) * cx[m]
                    plain = term if plain is None else plain + term
                flat_x[to, :] = row_of(planes, MINV, k) * x + plain
                flat_r[to, :] = r
                return carry

            for start, stop, seen in plan.reached(owner, first, last):
                over_rows(start, stop, functools.partial(step, seen=seen), 0, 4)
        for copy in departures[part]:
            copy.start()
    for copies in departures:
        for copy in copies:
            copy.wait()


def body(load_currents, labels, bump_height, horizontal_class, vertical_class, pad_class, edge_table, pad_table):
    rows, cols = labels.shape
    loads = load_currents.shape[0]
    nr, nc = lax.axis_size("row"), lax.axis_size("col")
    height, width = nr * rows // REG, nc * cols // REG
    plan = Plan(rows, cols, loads, height, width, nr, nc)
    n, regions, count = loads, REG * REG, plan.count
    field = (rows * n, cols)
    tall = ((rows + 2) * n, cols)
    edge = (4, 8, cols)
    sums = (2, LANES, cols)
    spread = (6 * plan.levels * n + 2 * n, cols)

    def vm(*dims):
        return pltpu.VMEM(dims, F32)

    def whole(*dims):
        return pltpu.VMEM(dims, jnp.int32)

    def sm(dims):
        return pltpu.SMEM(dims, F32)

    def dma(*dims):
        return pltpu.SemaphoreType.DMA(dims)

    legs = 4 * 6 + 3 * 8
    bt, b1, b2, planes, cx = pl.pallas_call(
        functools.partial(front_kernel, plan),
        out_shape=(shape(*field), shape(*field), shape(*field), shape(KEPT, rows, cols), shape(*spread)),
        in_specs=[HBM] * 8,
        out_specs=(HBM,) * 5,
        scratch_shapes=[
            whole(rows, cols), whole(rows, cols), whole(rows, cols), vm(rows, cols), whole(rows, cols), sm(edge_table.shape), sm(pad_table.shape),
            vm(n * plan.pitch, cols), vm(*field), vm(*tall), vm(*tall), vm(*field), vm(*field), vm(PLANES, rows, cols),
            vm(*edge), vm(*edge), vm(*edge), vm(*edge), vm(*edge), vm(*edge),
            vm(2, n, cols), vm(2, n, cols), vm(2, n, cols), vm(2, n, cols), vm(2, n, cols), vm(*field),
        ] + [vm(*sums)] * 8 + [
            vm(LANES, LANES),
            vm(2, 8, LANES), vm(4, 8, LANES), vm(2, 8, LANES), vm(2, 8, LANES), vm(2, 8, LANES), vm(2, 8, LANES),
            vm(2, 2, 8, LANES), vm(2, 4, 8, LANES), vm(2, 2, 8, LANES), vm(6, 8, LANES), vm(6, 8, LANES), vm(6, 8, LANES),
            vm(3, 8, LANES), vm(3, count, 8, LANES), vm(regions, LANES), vm(regions, LANES), vm(regions, LANES),
            vm(regions + 16, LANES), vm(regions + 16, LANES), vm(9, regions, LANES), vm(regions + LANES + 2 * REG, LANES), vm(*spread),
            pltpu.SemaphoreType.DMA, dma(7), dma(5), dma(20), dma(legs), dma(3), dma(3),
        ],
        compiler_params=pltpu.CompilerParams(collective_id=0, has_side_effects=True, vmem_limit_bytes=56 * 1024 * 1024),
    )(load_currents.reshape(n * rows, cols), horizontal_class, vertical_class, labels, bump_height, pad_class, edge_table, pad_table)
    staged = (n, plan.pitch, cols)
    return pl.pallas_call(
        functools.partial(last_kernel, plan),
        out_shape=(shape(n, rows, cols),) * 2,
        in_specs=[HBM] * 5,
        out_specs=(HBM, HBM),
        scratch_shapes=[
            vm(*field), vm(*field), vm(*field), vm(KEPT, rows, cols), vm(*staged), vm(*staged), vm(*spread),
            dma(plan.parts + 2, 4), dma(plan.parts + 2, 2), pltpu.SemaphoreType.DMA,
        ],
        compiler_params=pltpu.CompilerParams(vmem_limit_bytes=56 * 1024 * 1024),
    )(bt, b1, b2, planes, cx)


def solution(mesh):
    grid = P("row", "col")
    cube = P(None, "row", "col")
    return jax.shard_map(
        body,
        mesh=mesh,
        in_specs=(cube, grid, grid, grid, grid, grid, P(), P()),
        out_specs=(cube, cube),
        check_vma=False,
    )
```
